256 devices in a mesh: gx: 4 (over x), gy: 16 (over z_lo, y), gz: 4 (over z_hi, core).
Axes of the slice: x: 4, y: 4, z: 8 (z_hi: 2, z_lo: 4; z = z_hi * 4 + z_lo), core: 2. Of those that a mesh axis runs over, the one named last changes fastest.
Arguments:
- atom_embedding: bfloat16 [4, 16, 4, 64, 512], P('gx', 'gy', 'gz'), may hold values from -6 to 6
- output_adjoint: bfloat16 [4, 16, 4, 64, 512], P('gx', 'gy', 'gz'), may hold values from -6 to 6
- fractional_coords: float32 [4, 16, 4, 3, 512], P('gx', 'gy', 'gz'), may hold values from 0 to 1, as said below
- element_labels: int32 [4, 16, 4, 512], P('gx', 'gy', 'gz'), may hold values from 0 to 3
- adjacent_ghost_entries: int32 [4, 16, 4, 16, 512], P('gx', 'gy', 'gz'), may hold values from 0 to 13823, as said below
- miller_triples: int32 [3, 2048], replicated, may hold values from -8 to 8
- reciprocal_kernel: float32 [2048, 64], replicated, may hold values from 0.02 to 0.2
- channel_mixing_matrix: bfloat16 [64, 64], replicated, may hold values from -0.75 to 0.75
- element_channel_factor: float32 [4, 64], replicated, may hold values from 0.25 to 1.75
- distance_kernel: float32 [16, 64], replicated, may hold values from -1.5 to 1.5
Outputs:
- atom_grad: bfloat16 [4, 16, 4, 64, 512], P('gx', 'gy', 'gz')
- position_grad: float32 [4, 16, 4, 3, 512], P('gx', 'gy', 'gz')
- weight_grad: float32 [64, 64], replicated
- radial_grad: float32 [16, 64], replicated
- filter_grad: float32 [2048, 64], P(('gx', 'gy', 'gz'))
The draws below stay inside these ranges and needn't reach their ends.
Inputs may be any that keep to these rules, and one draw needn't show every extreme that they name: `adjacent_ghost_entries`: the atoms of a brick form 32 blocks of 16 in order; block q < 27 is the cell of offset (q // 9 - 1, (q // 3) % 3 - 1, q % 3 - 1) of the brick, blocks 27 to 31 lie in its central cell. A ghost entry e names atom e % 512 of slot e // 512; an entry in a slot of offset o names an atom of a block whose cell offset equals -o in every dimension where o is not zero, and o is zero in every dimension where the listing atom's cell offset is zero; every slot occurs. `fractional_coords`: an atom of a block whose cell offset is -1 or 1 in a dimension lies within a quarter of the brick length of that face in that dimension. `miller_triples`: integer components; any triple may occur, the zero triple too.
All inputs are finite; a program needn't handle non-finite values.
Results may differ from the reference program's by a relative error of at most 0.0053.
Values may be sent and summed in bfloat16 or wider, within the bound.
A program may use at most 128 MiB of HBM per device.

```python
import math
import jax
import jax.numpy as jnp
from jax import lax

ATOMS_DEV = 512
CH = 64
RECIP_POINTS = 2048
NBR = 16
NB = 16
KINDS = 4
MAX_RECIP_INDEX = 8
GX = 4
GY = 16
GZ = 4
N_GX = 4
N_GY = 16
N_GZ = 4


rim_width = 0.25


def block_cells():
    block_ids = jnp.arange(32, dtype=jnp.int32)
    first = jnp.where(block_ids < 27, block_ids // 9 - 1, 0)
    second = jnp.where(block_ids < 27, block_ids // 3 % 3 - 1, 0)
    third = jnp.where(block_ids < 27, block_ids % 3 - 1, 0)
    return jnp.stack([first, second, third], axis=1)


def atom_cells():
    atom_ids = jnp.arange(ATOMS_DEV, dtype=jnp.int32)
    return block_cells()[atom_ids // (ATOMS_DEV // 32)]


def draw_fractional_coords(key, part):
    cells = jnp.transpose(atom_cells(), (1, 0))
    uniform_part = jax.random.uniform(key, (GX, GY, GZ, 3, ATOMS_DEV), jnp.float32)
    low_side = rim_width * uniform_part
    high_side = 1.0 - rim_width + rim_width * uniform_part
    middle = rim_width + (1.0 - 2.0 * rim_width) * uniform_part
    return jnp.where(cells == -1, low_side, jnp.where(cells == 1, high_side, middle)).astype(jnp.float32)


def draw_adjacent_ghost_entries(key, part):
    key_cross = jax.random.fold_in(key, 11)
    key_centre = jax.random.fold_in(key, 12)
    key_atom = jax.random.fold_in(key, 13)
    array_dimensions = (GX, GY, GZ, NBR, ATOMS_DEV)
    cell_atoms = ATOMS_DEV // 32
    own_cell = jnp.transpose(atom_cells(), (1, 0))
    crossing = jax.random.randint(key_cross, (GX, GY, GZ, NBR, 3, ATOMS_DEV), 0, 2).astype(jnp.int32)
    offsets = own_cell * crossing
    target = jnp.where(offsets != 0, -own_cell, own_cell)
    slot_id = 9 * (offsets[:, :, :, :, 0] + 1) + 3 * (offsets[:, :, :, :, 1] + 1) + (offsets[:, :, :, :, 2] + 1)
    drawn_block = 9 * (target[:, :, :, :, 0] + 1) + 3 * (target[:, :, :, :, 1] + 1) + (target[:, :, :, :, 2] + 1)
    centre_pick = jax.random.randint(key_centre, array_dimensions, 0, 6).astype(jnp.int32)
    centre_block = jnp.where(centre_pick == 0, 13, 26 + centre_pick)
    target_block = jnp.where(drawn_block == 13, centre_block, drawn_block)
    atom_pick = jax.random.randint(key_atom, array_dimensions, 0, cell_atoms).astype(jnp.int32)
    return (slot_id * ATOMS_DEV + target_block * cell_atoms + atom_pick).astype(jnp.int32)


def touch_ends(drawn, rng, least, largest):
    index_at = [jax.random.randint(jax.random.fold_in(rng, axis), (), 0, length) for axis, length in enumerate(drawn.shape)]
    widest = drawn.shape.index(max(drawn.shape))
    neighbour = index_at[:widest] + [(index_at[widest] + 1) % drawn.shape[widest]] + index_at[widest + 1:]
    return drawn.at[tuple(index_at)].set(least).at[tuple(neighbour)].set(largest)


def level_of(own_key, shape, cuts, least, high):
    level = 1.0
    for axis_at, blocks in cuts:
        steps = jax.random.uniform(jax.random.fold_in(jax.random.fold_in(own_key, 6), axis_at), (blocks,), jnp.float32, least / len(cuts), high / len(cuts))
        level = level * jnp.repeat(jnp.exp(steps), shape[axis_at] // blocks).reshape((-1,) + (1,) * (len(shape) - 1 - axis_at))
    return level


def centred(key, shape, scale, bound, pieces=(), kind=jnp.bfloat16):
    result = jax.random.normal(key, shape, jnp.float32) * scale
    if len(pieces) > 0:
        result = level_of(key, shape, pieces, -0.22, 0.18) * result
    return jnp.clip(result, min=-bound, max=bound).astype(kind)


def setup_inputs(seed: int = 0) -> dict:
    arg_keys = jax.random.split(jax.random.key(seed), 11)
    return {
        "atom_embedding": centred(arg_keys[0], (GX, GY, GZ, CH, ATOMS_DEV), 1.0, 6.0, ((0, 4), (1, 16), (2, 4))),
        "output_adjoint": centred(arg_keys[1], (GX, GY, GZ, CH, ATOMS_DEV), 1.0, 6.0, ((0, 4), (1, 16), (2, 4))),
        "fractional_coords": draw_fractional_coords(jax.random.fold_in(arg_keys[10], 71), 0),
        "element_labels": touch_ends(jax.random.randint(arg_keys[3], (GX, GY, GZ, ATOMS_DEV), 0, KINDS), jax.random.fold_in(arg_keys[3], 1), 0, KINDS - 1).astype(jnp.int32),
        "adjacent_ghost_entries": draw_adjacent_ghost_entries(jax.random.fold_in(arg_keys[10], 71), 0),
        "miller_triples": touch_ends(jax.random.randint(arg_keys[5], (3, RECIP_POINTS), 0 - MAX_RECIP_INDEX, MAX_RECIP_INDEX + 1), jax.random.fold_in(arg_keys[5], 1), 0 - MAX_RECIP_INDEX, MAX_RECIP_INDEX).astype(jnp.int32),
        "reciprocal_kernel": jnp.clip(jnp.exp(jax.random.uniform(arg_keys[6], (RECIP_POINTS, CH), jnp.float32, math.log(0.02), math.log(0.2))), 0.02, 0.2),
        "channel_mixing_matrix": centred(arg_keys[7], (CH, CH), CH ** -0.5, 0.75),
        "element_channel_factor": jnp.clip(1.0 + 0.15 * jax.random.normal(arg_keys[8], (KINDS, CH), jnp.float32), 0.25, 1.75),
        "distance_kernel": centred(arg_keys[9], (NB, CH), NB ** -0.5, 1.5, (), jnp.float32),
    }


circle_angle = 2.0 * math.pi
reach_sq = 0.75

def phases(local_pos, anchor, reciprocal_points_rescaled):
    absolute = local_pos + anchor[:, None]
    angles = absolute[0][:, None] * reciprocal_points_rescaled[0][None, :]
    angles = angles + absolute[1][:, None] * reciprocal_points_rescaled[1][None, :]
    angles = angles + absolute[2][:, None] * reciprocal_points_rescaled[2][None, :]
    return (jnp.cos(angles).astype(jnp.bfloat16), jnp.sin(angles).astype(jnp.bfloat16))

def structure_terms(cos_part, sin_part, stacked):
    contract = (((0,), (1,)), ((), ()))
    with_cos = lax.dot_general(cos_part, stacked, contract, preferred_element_type=jnp.float32)
    with_sin = lax.dot_general(sin_part, stacked, contract, preferred_element_type=jnp.float32)
    return jnp.concatenate([with_cos, with_sin], axis=1)

def coefficients(totals, filt_rows, norm_atoms, norm_k):
    channels = filt_rows.shape[1]
    cos_struct = totals[:, 0:channels] * norm_atoms
    cos_back = totals[:, channels:2 * channels] * norm_k
    sin_struct = totals[:, 2 * channels:3 * channels] * norm_atoms
    sin_back = totals[:, 3 * channels:4 * channels] * norm_k
    coeffs = jnp.concatenate([norm_atoms * filt_rows * cos_back, norm_k * filt_rows * cos_struct, norm_atoms * filt_rows * sin_back, norm_k * filt_rows * sin_struct], axis=1)
    return (coeffs.astype(jnp.bfloat16), cos_struct * cos_back + sin_struct * sin_back)

def ewald_pieces(running, piece_rows, start_at, cos_all, sin_all, stacked, reciprocal_points_rescaled):
    count_rows = piece_rows.shape[0]
    channels = stacked.shape[0] // 2
    cos_part = lax.dynamic_slice_in_dim(cos_all, start_at, count_rows, 1)
    sin_part = lax.dynamic_slice_in_dim(sin_all, start_at, count_rows, 1)
    kv_part = lax.dynamic_slice_in_dim(reciprocal_points_rescaled, start_at, count_rows, 1)
    contract = (((0,), (1,)), ((), ()))
    atom_part = lax.dot_general(piece_rows[:, 0:channels], cos_part, contract, preferred_element_type=jnp.float32)
    atom_part = atom_part + lax.dot_general(piece_rows[:, 2 * channels:3 * channels], sin_part, contract, preferred_element_type=jnp.float32)
    along_u = lax.dot_general(stacked, piece_rows[:, 0:2 * channels], contract, preferred_element_type=jnp.float32)
    along_v = lax.dot_general(stacked, piece_rows[:, 2 * channels:4 * channels], contract, preferred_element_type=jnp.float32)
    angle_grad = along_v * cos_part.astype(jnp.float32) - along_u * sin_part.astype(jnp.float32)
    pos_part = lax.dot_general(kv_part, angle_grad, (((1,), (1,)), ((), ())), precision=lax.Precision.HIGHEST)
    return (running[0] + atom_part, running[1] + pos_part)

def species_gains(table, kinds):
    onehot = (kinds[None, :] == jnp.arange(table.shape[0], dtype=jnp.int32)[:, None]).astype(jnp.float32)
    return lax.dot_general(table, onehot, (((0,), (0,)), ((), ())), precision=lax.Precision.HIGHEST)

def offset_table():
    steps_one = jnp.arange(3, dtype=jnp.float32) - 1.0
    along_x = jnp.broadcast_to(steps_one[:, None, None], (3, 3, 3))
    along_y = jnp.broadcast_to(steps_one[None, :, None], (3, 3, 3))
    along_z = jnp.broadcast_to(steps_one[None, None, :], (3, 3, 3))
    return jnp.stack([along_x, along_y, along_z], axis=-1)

def short_range(ghost_values, ghost_places, neighbour_ids, radial_weights):
    channels = ghost_values.shape[1]
    flat_z = jnp.transpose(ghost_values, (1, 0, 2)).reshape(channels, -1)
    flat_pos = jnp.transpose(ghost_places, (1, 0, 2)).reshape(3, -1)
    near_z = flat_z[:, neighbour_ids]
    near_pos = flat_pos[:, neighbour_ids]
    relative = near_pos - ghost_places[13][:, None, :]
    dist_sq = lax.optimization_barrier(jnp.sum(relative * relative, axis=0))
    basis_count = radial_weights.shape[0]
    spacing = reach_sq / (basis_count - 1)
    centres = jnp.arange(basis_count, dtype=jnp.float32) * spacing
    radial_basis = jnp.exp(-jnp.square((dist_sq[None, :, :] - centres[:, None, None]) / (2.0 * spacing)))
    filters = jnp.einsum('bc,bja->cja', radial_weights, radial_basis, precision=lax.Precision.HIGHEST)
    agg = lax.optimization_barrier(jnp.sum(filters * near_z, axis=1)) * neighbour_ids.shape[0] ** (-0.5)
    return jax.nn.silu(agg)

def local_backward(ghost_z, ghost_pos, neighbour_ids, distance_kernel, upstream):

    def mapped(ghost_values, ghost_places, radial_weights):
        return short_range(ghost_values, ghost_places, neighbour_ids, radial_weights)
    _, pullback = jax.vjp(mapped, ghost_z.astype(jnp.float32), ghost_pos, distance_kernel)
    return pullback(upstream.astype(jnp.float32))

def fold_wrap(padded, along_axis):
    inner_size = padded.shape[along_axis] - 2
    interior = lax.slice_in_dim(padded, 1, inner_size + 1, axis=along_axis)
    low_plane = lax.slice_in_dim(padded, 0, 1, axis=along_axis)
    high_plane = lax.slice_in_dim(padded, inner_size + 1, inner_size + 2, axis=along_axis)
    middle_shape = list(low_plane.shape)
    middle_shape[along_axis] = inner_size - 2
    middle = jnp.zeros(middle_shape, padded.dtype)
    return interior + jnp.concatenate([high_plane, middle, low_plane], axis=along_axis)

def reference(atom_embedding, output_adjoint, fractional_coords, element_labels, adjacent_ghost_entries, miller_triples, reciprocal_kernel, channel_mixing_matrix, element_channel_factor, distance_kernel):
    brick_count = N_GX * N_GY * N_GZ
    atom_count = ATOMS_DEV
    norm_atoms = (atom_count * brick_count) ** (-0.5)
    norm_k = RECIP_POINTS ** (-0.5)
    accumulated_entries = jnp.array([N_GX, N_GY, N_GZ], jnp.float32)
    reciprocal_points_rescaled = miller_triples.astype(jnp.float32) * (circle_angle / accumulated_entries)[:, None]
    flat_h = atom_embedding.reshape(brick_count, CH, atom_count)
    flat_dy = output_adjoint.reshape(brick_count, CH, atom_count)
    flat_pos = fractional_coords.reshape(brick_count, 3, atom_count)
    flat_kind = element_labels.reshape(brick_count, atom_count)
    flat_nbr = adjacent_ghost_entries.reshape(brick_count, NBR, atom_count)
    indices = jnp.arange(brick_count, dtype=jnp.int32)

    def locate(brick_id):
        brick_id = brick_id.astype(jnp.int32)
        return ((brick_id // (N_GY * N_GZ)).astype(jnp.int32), (brick_id // N_GZ % N_GY).astype(jnp.int32), (brick_id % N_GZ).astype(jnp.int32))

    def anchor_of(brick_id):
        brick_x, brick_y, brick_z = locate(brick_id)
        return jnp.stack([brick_x, brick_y, brick_z]).astype(jnp.float32)

    def add_terms(totals, brick_id):
        cos_all, sin_all = phases(flat_pos[brick_id], anchor_of(brick_id), reciprocal_points_rescaled)
        stacked = jnp.concatenate([flat_h[brick_id], flat_dy[brick_id]], axis=0)
        return (totals + structure_terms(cos_all, sin_all, stacked), None)
    totals, _ = lax.scan(add_terms, jnp.zeros((RECIP_POINTS, 4 * CH), jnp.float32), indices)
    coeffs, filter_grad = coefficients(totals, reciprocal_kernel, norm_atoms, norm_k)

    def make_z(brick_id):
        gain_rows = species_gains(element_channel_factor, flat_kind[brick_id])
        projected = lax.dot_general(channel_mixing_matrix, flat_h[brick_id], (((0,), (0,)), ((), ())), preferred_element_type=jnp.float32)
        return ((projected * gain_rows).astype(jnp.bfloat16), gain_rows)
    zfeat, gains_all = lax.map(make_z, indices)
    pad_spec = ((1, 1), (1, 1), (1, 1), (0, 0), (0, 0))
    z_pad = jnp.pad(zfeat.reshape(N_GX, N_GY, N_GZ, CH, atom_count), pad_spec, mode='wrap')
    p_pad = jnp.pad(fractional_coords, pad_spec, mode='wrap')
    offsets = offset_table()[..., None]

    def brick_step(running, brick_id):
        grad_zpad, grad_ppad, grad_rad = running
        brick_x, brick_y, brick_z = locate(brick_id)
        zero_index = jnp.zeros((), jnp.int32)
        corner = (brick_x, brick_y, brick_z, zero_index, zero_index)
        ghost_z = lax.dynamic_slice(z_pad, corner, (3, 3, 3, CH, atom_count)).reshape(27, CH, atom_count)
        ghost_p = (lax.dynamic_slice(p_pad, corner, (3, 3, 3, 3, atom_count)) + offsets).reshape(27, 3, atom_count)
        grad_z, grad_p, grad_r = local_backward(ghost_z, ghost_p, flat_nbr[brick_id], distance_kernel, flat_dy[brick_id])
        region_z = lax.dynamic_slice(grad_zpad, corner, (3, 3, 3, CH, atom_count)) + grad_z.reshape(3, 3, 3, CH, atom_count)
        grad_zpad = lax.dynamic_update_slice(grad_zpad, region_z, corner)
        region_p = lax.dynamic_slice(grad_ppad, corner, (3, 3, 3, 3, atom_count)) + grad_p.reshape(3, 3, 3, 3, atom_count)
        grad_ppad = lax.dynamic_update_slice(grad_ppad, region_p, corner)
        cos_all, sin_all = phases(flat_pos[brick_id], anchor_of(brick_id), reciprocal_points_rescaled)
        stacked = jnp.concatenate([flat_h[brick_id], flat_dy[brick_id]], axis=0)
        zeros_pair = (jnp.zeros((CH, atom_count), jnp.float32), jnp.zeros((3, atom_count), jnp.float32))
        ewald_h, ewald_pos = ewald_pieces(zeros_pair, coeffs, zero_index, cos_all, sin_all, stacked, reciprocal_points_rescaled)
        return ((grad_zpad, grad_ppad, grad_rad + grad_r), (ewald_h, ewald_pos))
    start_state = (jnp.zeros((N_GX + 2, N_GY + 2, N_GZ + 2, CH, atom_count), jnp.float32), jnp.zeros((N_GX + 2, N_GY + 2, N_GZ + 2, 3, atom_count), jnp.float32), jnp.zeros((NB, CH), jnp.float32))
    (grad_zpad, grad_ppad, radial_grad), (ewald_h, ewald_pos) = lax.scan(brick_step, start_state, indices)
    zgrad = fold_wrap(fold_wrap(fold_wrap(grad_zpad, 0), 1), 2).reshape(brick_count, CH, atom_count)
    pos_short = fold_wrap(fold_wrap(fold_wrap(grad_ppad, 0), 1), 2).reshape(brick_count, 3, atom_count)
    zscaled = (zgrad * gains_all).astype(jnp.bfloat16)

    def finish(brick_id):
        atom_short = jnp.dot(channel_mixing_matrix, zscaled[brick_id], preferred_element_type=jnp.float32)
        atom_total = (flat_dy[brick_id].astype(jnp.float32) + ewald_h[brick_id] + atom_short).astype(jnp.bfloat16)
        weight_part = lax.dot_general(flat_h[brick_id], zscaled[brick_id], (((1,), (1,)), ((), ())), preferred_element_type=jnp.float32)
        return (atom_total, weight_part)
    atom_grad, weight_parts = lax.map(finish, indices)
    weight_grad = lax.optimization_barrier(jnp.sum(weight_parts, axis=0))
    position_grad = (ewald_pos + pos_short).reshape(fractional_coords.shape)
    return (atom_grad.reshape(atom_embedding.shape), position_grad, weight_grad, radial_grad, filter_grad)
```

```python
import functools
import math

import jax
import jax.numpy as jnp
from jax import lax
from jax.experimental import pallas as pl
from jax.experimental.pallas import tpu as pltpu
from jax.sharding import Mesh
from jax.sharding import PartitionSpec as P

AXES = ("gx", "gy_0", "gy_1", "gz_0", "gz_1")
GY = ("gy_0", "gy_1")
GZ = ("gz_0", "gz_1")
MESH = pl.DeviceIdType.MESH
f32, bf16, i32 = jnp.float32, jnp.bfloat16, jnp.int32

CH = 64
ATOMS = 512
NBR = 16
NB = 16
ROWS = 8
SEG = 768
FEAT = 80
reach_sq = 0.75

COS = (
    0.9999999890590228,
    -19.739204499454026,
    64.93911745990036,
    -85.45013953095037,
    60.16763095136588,
    -25.96759924965491,
    6.528658162567069,
)
SIN = (
    6.283185302511503,
    -41.34170040531769,
    81.60513138580204,
    -76.7030153539128,
    42.02592698618416,
    -14.899846668691637,
    3.238137510515757,
)

SLOTS = [(ox, oy, oz) for ox in (-1, 0, 1) for oy in (-1, 0, 1) for oz in (-1, 0, 1)]
FACES = [o for o in SLOTS if sum(map(abs, o)) == 1]
EDGES = [o for o in SLOTS if sum(map(abs, o)) == 2]
CORNERS = [o for o in SLOTS if sum(map(abs, o)) == 3]
GHOSTS = FACES + EDGES + CORNERS


def base_block(o):
    if o in FACES:
        return 32 + 9 * FACES.index(o)
    if o in EDGES:
        return 32 + 54 + 3 * EDGES.index(o)
    if o in CORNERS:
        return 32 + 54 + 36 + CORNERS.index(o)
    return 0


def poly(coef, x):
    acc = jnp.full_like(x, coef[-1])
    for c in coef[-2::-1]:
        acc = acc * x + c
    return acc


def split2(x):
    hi = x.astype(bf16)
    return hi, (x - hi.astype(f32)).astype(bf16)


def dot_nn(a, b):
    return jnp.dot(a, b, preferred_element_type=f32)


def dot_nt(a, b):
    return lax.dot_general(a, b, (((1,), (1,)), ((), ())), preferred_element_type=f32)


def pick(ref, o):
    return ref.at[tuple(slice(None) if c == 0 else 1 - c for c in o)]


def region(o, faces, edges, corners):
    if o in FACES:
        return faces.at[FACES.index(o)]
    if o in EDGES:
        return edges.at[EDGES.index(o)]
    return corners.at[CORNERS.index(o)]


def kernel(
    sizes,
    h_ref, dy_ref, pos_ref, lab_ref, idx_ref, mil_ref, kf_ref, mix_ref, gain_ref, rad_ref,
    atom_out, pos_out, weight_out, radial_out, filter_out,
    cs, tot, arr,
    feat, feat5, gf, ge, gc,
    meta, onehot, near, filt, basis_s, rel_s, dgs, agg_s, grad_s, own_s, ownpos_s, u_s, drad_s,
    sf, se, sc, rf, re, rc,
    rec_a, a_bf, rec_b, sum_b, rec_c, g1,
    m9_s, p9_s, st_s, stt_s, gains_s, ew_s, ep_s, kf_s, mi_s, tab_s,
    ar_l, ar_r, ar_x, ar_z, ar_o,
    kf_sem, gs, gr, bs, br, cs_s, cs_r, xs, xr, zs, zr, azs, azr, axs, axr, acs, acr,
    rcs, rcr, rxs, rxr, rzs, rzr, ros, ror,
):
    nx, nl, ny, nh, nc = sizes
    x, zl, y, zh, co = (lax.axis_index(a) for a in AXES)
    devices = nx * nl * ny * nh * nc
    gy, gz = zl * ny + y, zh * nc + co
    n_gy, n_gz = nl * ny, nh * nc
    owner = ((x * nl + zl) * ny + y) * nh * nc + zh * nc + co
    norm_atoms = (ATOMS * devices) ** (-0.5)
    norm_k = (ROWS * devices) ** (-0.5)

    def brick(ox, oy, oz):
        bx = lax.rem(x + (ox + nx), nx)
        by = lax.rem(gy + (oy + n_gy), n_gy)
        bz = lax.rem(gz + (oz + n_gz), n_gz)
        return (bx, by // ny, lax.rem(by, ny), bz // nc, lax.rem(bz, nc))

    xy_steps = [(i, j) for i in range(nx) for j in range(ny) if (i, j) != (0, 0)]
    z_steps = [(i, j) for i in range(nh) for j in range(nl) if (i, j) != (0, 0)]

    def xy_to(step):
        return lax.rem(x + step[0], nx), lax.rem(y + step[1], ny)

    def z_to(step):
        return lax.rem(zh + step[0], nh), lax.rem(zl + step[1], nl)

    sibling = (x, zl, y, zh, nc - 1 - co)

    def xy_dev(step):
        tx, ty = xy_to(step)
        return (tx, zl, ty, zh, co)

    def z_dev(step):
        th, tl = z_to(step)
        return (x, tl, y, th, co)

    def send(src, dst, ssem, rsem, dev):
        copy = pltpu.make_async_remote_copy(
            src_ref=src, dst_ref=dst, send_sem=ssem, recv_sem=rsem, device_id=dev, device_id_type=MESH
        )
        copy.start()
        return copy

    kf_copy = pltpu.make_async_copy(kf_ref.at[pl.ds(pl.multiple_of(owner * ROWS, ROWS), ROWS)], kf_s, kf_sem)
    kf_copy.start()

    barrier = pltpu.get_barrier_semaphore()
    partners = [brick(*o) for o in GHOSTS] + [xy_dev(s) for s in xy_steps] + [z_dev(s) for s in z_steps] + [sibling]
    for dev in partners:
        pl.semaphore_signal(barrier, inc=1, device_id=dev, device_id_type=MESH)

    hb = h_ref[...]
    tab_s[...] = jnp.zeros((8, 128), f32)
    tab_s[0:4, 0:CH] = gain_ref[...]
    tab = jnp.transpose(tab_s[...])[0:CH]
    lab = lab_ref[...]
    gains = jnp.zeros((CH, ATOMS), f32)
    for s in range(4):
        gains = jnp.where(lab == s, tab[:, s : s + 1], gains)
    gains_s[...] = gains
    mix = mix_ref[...]
    mix_t = jnp.transpose(mix.astype(f32)).astype(bf16)
    z = (dot_nn(mix_t, hb) * gains).astype(bf16).astype(f32)
    p = pos_ref[...]
    p_hi = p.astype(bf16).astype(f32)
    p_mid = (p - p_hi).astype(bf16).astype(f32)
    p_lo = (p - p_hi - p_mid).astype(bf16).astype(f32)
    rows = jnp.concatenate([z, p_hi, p_mid, p_lo, jnp.zeros((55, ATOMS), f32)], axis=0)
    rows = jnp.transpose(rows).astype(bf16)
    feat[...] = rows[0:432].reshape(3, 3, 3, 16, 128)
    feat5[...] = rows[432:512].reshape(5, 16, 128)

    pl.semaphore_wait(barrier, len(partners))
    ghost_copies = [
        send(pick(feat, o), region(o, gf, ge, gc), gs.at[n], gr.at[n], brick(-o[0], -o[1], -o[2]))
        for n, o in enumerate(GHOSTS)
    ]

    st = jnp.concatenate([hb, dy_ref[...]], axis=0)
    st_s[...] = st
    stt_s[...] = jnp.transpose(st.astype(f32)).astype(bf16)
    mil = mil_ref[...].astype(f32)
    mrows = jnp.concatenate([mil, mil, mil, jnp.zeros((7, mil.shape[1]), f32)], axis=0)
    mi_s[...] = mrows.astype(bf16)
    m9_s[...] = jnp.transpose(mrows).astype(bf16)
    absolute = jnp.concatenate(
        [
            (p[0:1] + x.astype(f32)) * (1.0 / nx),
            (p[1:2] + gy.astype(f32)) * (1.0 / n_gy),
            (p[2:3] + gz.astype(f32)) * (1.0 / n_gz),
        ],
        axis=0,
    )
    w_hi = absolute.astype(bf16).astype(f32)
    w_mid = (absolute - w_hi).astype(bf16).astype(f32)
    w_lo = (absolute - w_hi - w_mid).astype(bf16).astype(f32)
    p9_s[...] = jnp.concatenate([w_hi, w_mid, w_lo, jnp.zeros((7, ATOMS), f32)], axis=0).astype(bf16)

    chunk = 16 if devices >= 16 else devices

    def phase_step(n, _):
        at = pl.multiple_of(n * (chunk * ROWS), chunk * ROWS)
        t = dot_nn(m9_s[pl.ds(at, chunk * ROWS), :], p9_s[...])
        t = t - jnp.floor(t + 0.5)
        sq = t * t
        cosine = poly(COS, sq).reshape(chunk, ROWS, ATOMS)
        sine = (t * poly(SIN, sq)).reshape(chunk, ROWS, ATOMS)
        both = jnp.concatenate([cosine, sine], axis=1).reshape(chunk * 2 * ROWS, ATOMS).astype(bf16)
        cs[pl.ds(pl.multiple_of(n * (chunk * 2 * ROWS), chunk * 2 * ROWS), chunk * 2 * ROWS), :] = both
        part = dot_nn(both, stt_s[...])
        tot[pl.ds(n * (chunk // nc), chunk // nc)] = part.reshape(chunk // nc, nc, 16, 128)
        return 0

    lax.fori_loop(0, devices // chunk, phase_step, 0)

    core_copy = send(tot.at[:, nc - 1 - co], rec_a, cs_s.at[0], cs_r.at[0], sibling)

    e = idx_ref[...]
    slot, atom = e >> 9, e & 511
    block = atom >> 4
    o1 = (slot * 57) >> 9
    o2 = ((slot - 9 * o1) * 11) >> 5
    o3 = slot - 9 * o1 - 3 * o2
    c1 = (block * 57) >> 9
    c2 = ((block - 9 * c1) * 11) >> 5
    c3 = block - 9 * c1 - 3 * c2
    place = jnp.zeros_like(e)
    for o_n, c_n in ((o1, c1), (o2, c2), (o3, c3)):
        place = jnp.where(o_n == 1, place * 3 + c_n, place)
    base = jnp.zeros_like(e)
    for n, o in enumerate(SLOTS):
        base = jnp.where(slot == n, base_block(o), base)
    row = jnp.where(slot == 13, block, base + place) * 16 + (atom & 15)
    segment = jnp.where(row >= 2 * SEG, 2, jnp.where(row >= SEG, 1, 0))
    low = row - SEG * segment
    for j in range(NBR):
        meta[j] = jnp.concatenate(
            [v[j : j + 1] for v in (low, segment, o1 - 1, o2 - 1, o3 - 1)] + [jnp.zeros((3, ATOMS), i32)], axis=0
        )

    core_copy.wait_recv()

    def core_sum(n, _):
        part = tot[pl.ds(n * (nl * ny * nh), nl * ny * nh), co] + rec_a[pl.ds(n * (nl * ny * nh), nl * ny * nh)]
        a_bf[n] = part.astype(bf16).reshape(nl, ny, nh, 16, 128)
        return 0

    lax.fori_loop(0, nx, core_sum, 0)

    xy_copies = []
    for n, s in enumerate(xy_steps):
        tx, ty = xy_to(s)
        xy_copies.append(send(a_bf.at[tx, :, ty], rec_b.at[n], xs.at[n], xr.at[n], xy_dev(s)))

    for c in ghost_copies:
        c.wait_recv()

    table = jnp.concatenate(
        [
            feat[...].reshape(432, 128),
            feat5[...].reshape(80, 128),
            gf[...].reshape(864, 128),
            ge[...].reshape(576, 128),
            gc[...].reshape(128, 128),
            jnp.zeros((224, 128), bf16),
        ],
        axis=0,
    ).astype(f32)
    table = jnp.concatenate(
        [jnp.transpose(table[k * SEG : (k + 1) * SEG])[0:FEAT] for k in range(3)], axis=0
    ).astype(bf16)
    rad = rad_ref[...]
    rad_hi, rad_lo = split2(rad)
    radt_hi, radt_lo = split2(jnp.transpose(rad))
    rad_fwd = jnp.concatenate([radt_hi, radt_hi, radt_lo], axis=1)
    rad_bwd = jnp.concatenate([rad_hi, rad_hi, rad_lo], axis=1)
    spacing = reach_sq / (NB - 1)
    centres = lax.broadcasted_iota(i32, (NB, ATOMS), 0).astype(f32) * spacing
    agg_s[...] = jnp.zeros((CH, ATOMS), f32)

    def forward_step(j, _):
        m = meta[j]
        low_j, seg_j = m[0:1], m[1:2]
        hot = jnp.where(lax.broadcasted_iota(i32, (SEG, ATOMS), 0) == low_j, 1.0, 0.0).astype(bf16)
        onehot[j] = hot
        got = dot_nn(table, hot)
        got = jnp.where(
            seg_j == 0, got[0:FEAT], jnp.where(seg_j == 1, got[FEAT : 2 * FEAT], got[2 * FEAT : 3 * FEAT])
        )
        nz = got[0:CH]
        near[j] = nz.astype(bf16)
        rest = got[CH:FEAT]
        near_pos = (rest[0:3] + rest[3:6]) + rest[6:9]
        rel = (near_pos + m[2:5].astype(f32)) - pos_ref[...]
        sq = rel * rel
        dist = sq[0:1] + sq[1:2] + sq[2:3]
        rel_s[j] = jnp.concatenate([rel, dist, jnp.zeros((4, ATOMS), f32)], axis=0)
        d = (dist - centres) / (2.0 * spacing)
        b = jnp.exp(-(d * d))
        basis_s[j] = b
        b_hi, b_lo = split2(b)
        fl = dot_nn(rad_fwd, jnp.concatenate([b_hi, b_lo, b_hi], axis=0))
        filt[j] = fl
        agg_s[...] += fl * nz
        return 0

    lax.fori_loop(0, NBR, forward_step, 0)

    v = agg_s[...] * NBR ** (-0.5)
    sig = 1.0 / (1.0 + jnp.exp(-v))
    u_s[...] = dy_ref[...].astype(f32) * (sig * (1.0 + v * (1.0 - sig))) * NBR ** (-0.5)

    for c in xy_copies:
        c.wait_recv()
    part = a_bf[x, :, y].astype(f32)
    for n in range(len(xy_steps)):
        part = part + rec_b[n].astype(f32)
    sum_b[...] = part

    z_copies = []
    for n, s in enumerate(z_steps):
        th, tl = z_to(s)
        z_copies.append(send(sum_b.at[tl, th], rec_c.at[n], zs.at[n], zr.at[n], z_dev(s)))

    grad_s[...] = jnp.zeros((SEG, 3 * FEAT), f32)
    ownpos_s[...] = jnp.zeros((8, ATOMS), f32)
    drad_s[...] = jnp.zeros((2 * NB, 2 * CH), f32)

    def backward_step(j, _):
        u = u_s[...]
        nz = near[j].astype(f32)
        dz = u * filt[j]
        df = u * nz
        df_hi, df_lo = split2(df)
        b = basis_s[j]
        b_hi, b_lo = split2(b)
        db = dot_nn(rad_bwd, jnp.concatenate([df_hi, df_lo, df_hi], axis=0))
        drad_s[...] += dot_nt(
            jnp.concatenate([b_hi, b_lo], axis=0), jnp.concatenate([df_hi, df_lo], axis=0)
        )
        r = rel_s[j]
        d = (r[3:4] - centres) / (2.0 * spacing)
        ddist = jnp.sum(db * b * d, axis=0, keepdims=True) * (-2.0 / (2.0 * spacing))
        drel = 2.0 * r[0:3] * ddist
        ownpos_s[0:3] += drel
        drel_hi = drel.astype(bf16).astype(f32)
        stack = jnp.concatenate([dz, drel_hi, drel - drel_hi, jnp.zeros((10, ATOMS), f32)], axis=0)
        seg_j = meta[j][1:2]
        dg = jnp.concatenate([jnp.where(seg_j == k, stack, 0.0) for k in range(3)], axis=0)
        dgs[...] = dg.astype(bf16)
        grad_s[...] += dot_nt(onehot[j], dgs[...])
        return 0

    half = NBR // 2
    lax.fori_loop(0, half, backward_step, 0)

    for c in z_copies:
        c.wait_recv()
    total = sum_b[zl, zh]
    for n in range(len(z_steps)):
        total = total + rec_c[n]
    kf_copy.wait()
    kf = kf_s[...]
    struct = total[:, 0:CH] * norm_atoms
    back = total[:, CH : 2 * CH] * norm_k
    prod = struct * back
    filter_out[...] = prod[0:ROWS] + prod[ROWS : 2 * ROWS]
    kf2 = jnp.concatenate([kf, kf], axis=0)
    coeffs = jnp.concatenate([norm_atoms * kf2 * back, norm_k * kf2 * struct], axis=1).astype(bf16)
    g1[zl, zh] = coeffs
    az_copies = [
        send(g1.at[zl, zh], g1.at[zl, zh], azs.at[n], azr.at[n], z_dev(s)) for n, s in enumerate(z_steps)
    ]

    lax.fori_loop(half, NBR, backward_step, 0)

    grad = grad_s[...]
    table_grad = jnp.concatenate(
        [
            jnp.concatenate([grad[:, k * FEAT : (k + 1) * FEAT], jnp.zeros((SEG, 128 - FEAT), f32)], axis=1)
            for k in range(3)
        ],
        axis=0,
    )
    own_s[...] = table_grad[0:512].reshape(32, 16, 128)
    sf[...] = table_grad[512:1376].astype(bf16).reshape(6, 3, 3, 16, 128)
    se[...] = table_grad[1376:1952].astype(bf16).reshape(12, 3, 16, 128)
    sc[...] = table_grad[1952:2080].astype(bf16).reshape(8, 16, 128)
    back_copies = [
        send(region(o, sf, se, sc), region(o, rf, re, rc), bs.at[n], br.at[n], brick(*o))
        for n, o in enumerate(GHOSTS)
    ]

    for c in az_copies:
        c.wait_recv()
    arr[x, :, y, :, co] = g1[...]
    ax_copies = [
        send(g1, arr.at[x, :, y, :, co], axs.at[n], axr.at[n], xy_dev(s)) for n, s in enumerate(xy_steps)
    ]

    for c in back_copies:
        c.wait_recv()
    for o in GHOSTS:
        got = region(o, rf, re, rc)[...].astype(f32)
        view = [range(3) if c == 0 else [1 - c] for c in o]
        got = got.reshape(-1, 16, 128)
        n = 0
        for i in view[0]:
            for k in view[1]:
                for l in view[2]:
                    own_s[9 * i + 3 * k + l] += got[n]
                    n += 1
    own = jnp.transpose(own_s[...].reshape(512, 128))
    gains = gains_s[...]
    zscaled = (own[0:CH] * gains).astype(bf16)
    pos_short = (own[64:67] + own[67:70]) - ownpos_s[0:3]
    ew_s[...] = dy_ref[...].astype(f32) + dot_nn(mix_ref[...], zscaled)
    weight = dot_nt(h_ref[...], zscaled)
    dr = drad_s[...]
    dr = dr[0:NB, 0:CH] + (dr[NB : 2 * NB, 0:CH] + dr[0:NB, CH : 2 * CH]) + dr[NB : 2 * NB, CH : 2 * CH]
    small = jnp.concatenate(
        [
            jnp.concatenate([weight[0:32], weight[32:64]], axis=1),
            jnp.concatenate([dr[0:8], dr[8:16]], axis=1),
            jnp.zeros((8, 128), f32),
        ],
        axis=0,
    )
    ar_l[...] = small.reshape(2, 24, 128)
    rc_copy = send(ar_l.at[nc - 1 - co], ar_r, rcs.at[0], rcr.at[0], sibling)

    for c in ax_copies:
        c.wait_recv()
    ac_copy = send(
        arr.at[:, :, :, :, co], arr.at[:, :, :, :, co], acs.at[0], acr.at[0], sibling
    )

    rc_copy.wait_recv()
    ar_x[x * ny + y] = ar_l[co] + ar_r[...]
    rx_copies = [
        send(ar_x.at[x * ny + y], ar_x.at[x * ny + y], rxs.at[n], rxr.at[n], xy_dev(s))
        for n, s in enumerate(xy_steps)
    ]
    ac_copy.wait_recv()

    ep_s[...] = jnp.zeros((16, ATOMS), f32)

    def ewald_step(n, _):
        rows_n = chunk * 2 * ROWS
        co_n = arr_chunk(n)
        cs_n = cs[pl.ds(pl.multiple_of(n * rows_n, rows_n), rows_n), :]
        along = dot_nn(co_n, st_s[...]).reshape(chunk, 2, ROWS, ATOMS)
        trig = cs_n.astype(f32).reshape(chunk, 2, ROWS, ATOMS)
        ag = (along[:, 1] * trig[:, 0] - along[:, 0] * trig[:, 1]).reshape(chunk * ROWS, ATOMS)
        ag_hi, ag_lo = split2(ag)
        m_n = mi_s[:, pl.ds(pl.multiple_of(n * (chunk * ROWS), chunk * ROWS), chunk * ROWS)]
        ep_s[...] += dot_nn(m_n, ag_hi) + dot_nn(m_n, ag_lo)
        co_t = jnp.transpose(co_n.astype(f32))[0:CH].astype(bf16)
        ew_s[...] += dot_nn(co_t, cs_n)
        return 0

    per_x = nl * ny * nh * nc // chunk

    def arr_chunk(n):
        i = n // per_x
        r = lax.rem(n, per_x)
        if nl * ny * nh * nc // nl == chunk:
            return arr[i, r].reshape(chunk * 16, 128)
        return arr[i].reshape(chunk * 16, 128)

    steps = devices // chunk
    lax.fori_loop(0, steps // 2, ewald_step, 0)

    for c in rx_copies:
        c.wait_recv()
    part = ar_x[0]
    for n in range(1, nx * ny):
        part = part + ar_x[n]
    ar_z[zl * nh + zh] = part
    rz_copies = [
        send(ar_z.at[zl * nh + zh], ar_z.at[zl * nh + zh], rzs.at[n], rzr.at[n], z_dev(s))
        for n, s in enumerate(z_steps)
    ]

    lax.fori_loop(steps // 2, steps, ewald_step, 0)
    atom_out[...] = ew_s[...].astype(bf16)
    ep = ep_s[0:3]
    turn = 2.0 * math.pi
    pos_out[...] = pos_short + jnp.concatenate(
        [ep[0:1] * (turn / nx), ep[1:2] * (turn / n_gy), ep[2:3] * (turn / n_gz)], axis=0
    )

    for c in rz_copies:
        c.wait_recv()
    part = ar_z[0]
    for n in range(1, nl * nh):
        part = part + ar_z[n]
    ar_o[co] = part
    ro_copy = send(ar_o.at[co], ar_o.at[co], ros.at[0], ror.at[0], sibling)
    ro_copy.wait_recv()
    full = ar_o[...].reshape(48, 128)
    weight_out[...] = jnp.concatenate([full[0:32, 0:CH], full[0:32, CH : 2 * CH]], axis=0)
    radial_out[...] = jnp.concatenate([full[32:40, 0:CH], full[32:40, CH : 2 * CH]], axis=0)

    for c in (
        ghost_copies + [core_copy] + xy_copies + z_copies + az_copies + ax_copies + back_copies
        + [rc_copy, ac_copy] + rx_copies + rz_copies + [ro_copy]
    ):
        c.wait_send()


def shards(sizes, h, dy, pos, labels, entries, miller, kfilter, mix, table, radial):
    nx, nl, ny, nh, nc = sizes
    devices = nx * nl * ny * nh * nc
    k = ROWS * devices
    nxy, nz = nx * ny, nl * nh
    vmem = pl.BlockSpec(memory_space=pltpu.VMEM)
    dma = pltpu.SemaphoreType.DMA
    plane = devices // nc
    scratch = [
        pltpu.VMEM((2 * k, ATOMS), bf16),
        pltpu.VMEM((plane, nc, 16, 128), f32),
        pltpu.VMEM((nx, nl, ny, nh, nc, 16, 128), bf16),
        pltpu.VMEM((3, 3, 3, 16, 128), bf16),
        pltpu.VMEM((5, 16, 128), bf16),
        pltpu.VMEM((6, 3, 3, 16, 128), bf16),
        pltpu.VMEM((12, 3, 16, 128), bf16),
        pltpu.VMEM((8, 16, 128), bf16),
        pltpu.VMEM((NBR, 8, ATOMS), i32),
        pltpu.VMEM((NBR, SEG, ATOMS), bf16),
        pltpu.VMEM((NBR, CH, ATOMS), bf16),
        pltpu.VMEM((NBR, CH, ATOMS), f32),
        pltpu.VMEM((NBR, NB, ATOMS), f32),
        pltpu.VMEM((NBR, 8, ATOMS), f32),
        pltpu.VMEM((3 * FEAT, ATOMS), bf16),
        pltpu.VMEM((CH, ATOMS), f32),
        pltpu.VMEM((SEG, 3 * FEAT), f32),
        pltpu.VMEM((32, 16, 128), f32),
        pltpu.VMEM((8, ATOMS), f32),
        pltpu.VMEM((CH, ATOMS), f32),
        pltpu.VMEM((2 * NB, 2 * CH), f32),
        pltpu.VMEM((6, 3, 3, 16, 128), bf16),
        pltpu.VMEM((12, 3, 16, 128), bf16),
        pltpu.VMEM((8, 16, 128), bf16),
        pltpu.VMEM((6, 3, 3, 16, 128), bf16),
        pltpu.VMEM((12, 3, 16, 128), bf16),
        pltpu.VMEM((8, 16, 128), bf16),
        pltpu.VMEM((plane, 16, 128), f32),
        pltpu.VMEM((nx, nl, ny, nh, 16, 128), bf16),
        pltpu.VMEM((nxy - 1, nl, nh, 16, 128), bf16),
        pltpu.VMEM((nl, nh, 16, 128), f32),
        pltpu.VMEM((nz - 1, 16, 128), f32),
        pltpu.VMEM((nl, nh, 16, 128), bf16),
        pltpu.VMEM((k, 16), bf16),
        pltpu.VMEM((16, ATOMS), bf16),
        pltpu.VMEM((2 * CH, ATOMS), bf16),
        pltpu.VMEM((ATOMS, 2 * CH), bf16),
        pltpu.VMEM((CH, ATOMS), f32),
        pltpu.VMEM((CH, ATOMS), f32),
        pltpu.VMEM((16, ATOMS), f32),
        pltpu.VMEM((ROWS, CH), f32),
        pltpu.VMEM((16, k), bf16),
        pltpu.VMEM((8, 128), f32),
        pltpu.VMEM((2, 24, 128), f32),
        pltpu.VMEM((24, 128), f32),
        pltpu.VMEM((nxy, 24, 128), f32),
        pltpu.VMEM((nz, 24, 128), f32),
        pltpu.VMEM((2, 24, 128), f32),
        dma,
    ]
    for count in (26, 26, 1, nxy - 1, nz - 1, nz - 1, nxy - 1, 1, 1, nxy - 1, nz - 1, 1):
        scratch += [dma((count,)), dma((count,))]
    out = pl.pallas_call(
        functools.partial(kernel, sizes),
        out_shape=(
            jax.ShapeDtypeStruct((CH, ATOMS), bf16),
            jax.ShapeDtypeStruct((3, ATOMS), f32),
            jax.ShapeDtypeStruct((CH, CH), f32),
            jax.ShapeDtypeStruct((NB, CH), f32),
            jax.ShapeDtypeStruct((ROWS, CH), f32),
        ),
        in_specs=[vmem] * 6 + [pl.BlockSpec(memory_space=pl.ANY)] + [vmem] * 3,
        out_specs=(vmem,) * 5,
        scratch_shapes=scratch,
        compiler_params=pltpu.CompilerParams(
            collective_id=0, has_side_effects=True, vmem_limit_bytes=60 * 1024 * 1024
        ),
        name="layer",
    )(
        h[0, 0, 0], dy[0, 0, 0], pos[0, 0, 0], labels[0, 0], entries[0, 0, 0],
        miller, kfilter, mix, table, radial,
    )
    return (out[0][None, None, None], out[1][None, None, None], out[2], out[3], out[4])


def solution(mesh):
    sizes = (mesh.shape["gx"], 4, mesh.shape["gy"] // 4, mesh.shape["gz"] // 2, 2)
    finer = Mesh(mesh.devices.reshape(sizes), AXES)
    brick = P("gx", GY, GZ, None, None)
    return jax.shard_map(
        functools.partial(shards, sizes),
        mesh=finer,
        in_specs=(brick, brick, brick, P("gx", GY, GZ, None), brick, P(), P(), P(), P(), P()),
        out_specs=(brick, brick, P(), P(), P(AXES, None)),
        check_vma=False,
    )
```

```python
import functools
import math

import jax
import jax.numpy as jnp
from jax import lax
from jax.experimental import pallas as pl
from jax.experimental.pallas import tpu as pltpu
from jax.sharding import Mesh
from jax.sharding import PartitionSpec as P

AXES = ("gx", "gy_0", "gy_1", "gz_0", "gz_1")
GY = ("gy_0", "gy_1")
GZ = ("gz_0", "gz_1")
MESH = pl.DeviceIdType.MESH
f32, bf16, i32 = jnp.float32, jnp.bfloat16, jnp.int32

CH = 64
ATOMS = 512
NBR = 16
NB = 16
ROWS = 8
SEG = 528
BLOCKS = 144
GROUP = 4
reach_sq = 0.75

COS = (
    0.9999999890590228,
    -19.739204499454026,
    64.93911745990036,
    -85.45013953095037,
    60.16763095136588,
    -25.96759924965491,
    6.528658162567069,
)
SIN = (
    6.283185302511503,
    -41.34170040531769,
    81.60513138580204,
    -76.7030153539128,
    42.02592698618416,
    -14.899846668691637,
    3.238137510515757,
)

SLOTS = [(ox, oy, oz) for ox in (-1, 0, 1) for oy in (-1, 0, 1) for oz in (-1, 0, 1)]
FACES = [o for o in SLOTS if sum(map(abs, o)) == 1]
EDGES = [o for o in SLOTS if sum(map(abs, o)) == 2]
CORNERS = [o for o in SLOTS if sum(map(abs, o)) == 3]
GHOSTS = FACES + EDGES + CORNERS


def base_block(o):
    if o in FACES:
        return 32 + 9 * FACES.index(o)
    if o in EDGES:
        return 32 + 54 + 3 * EDGES.index(o)
    if o in CORNERS:
        return 32 + 54 + 36 + CORNERS.index(o)
    return 0


def poly(coef, x):
    acc = jnp.full_like(x, coef[-1])
    for c in coef[-2::-1]:
        acc = acc * x + c
    return acc


def split2(x):
    hi = x.astype(bf16)
    return hi, (x - hi.astype(f32)).astype(bf16)


def split3(x):
    hi = x.astype(bf16)
    rest = x - hi.astype(f32)
    mid = rest.astype(bf16)
    return hi, mid, (rest - mid.astype(f32)).astype(bf16)


def dot_nn(a, b):
    return jnp.dot(a, b, preferred_element_type=f32)


def dot_nt(a, b):
    return lax.dot_general(a, b, (((1,), (1,)), ((), ())), preferred_element_type=f32)


def pick(ref, o):
    return ref.at[tuple(slice(None) if c == 0 else 1 - c for c in o)]


def region(o, faces, edges, corners):
    if o in FACES:
        return faces.at[FACES.index(o)]
    if o in EDGES:
        return edges.at[EDGES.index(o)]
    return corners.at[CORNERS.index(o)]


def kernel(
    sizes,
    h_ref, dy_ref, pos_ref, lab_ref, idx_ref, mil_ref, kf_ref, mix_ref, gain_ref, rad_ref,
    atom_out, pos_out, weight_out, radial_out, filter_out,
    cs, tot, arr,
    feat, feat5, gf, ge, gc,
    pfeat, pfeat5, pgf, pge, pgc, psf, pse, psc, prf, pre, prc, table_s, xp_s, hotb, dgp, gradp_s, ownp_s,
    meta, onehot, near, filt, basis_s, rel_s, dgs, agg_s, grad_s, own_s, ownpos_s, u_s, drad_s,
    sf, se, sc, rf, re, rc,
    rec_a, a_bf, rec_b, sum_b, rec_c, g1,
    m9_s, p9_s, st_s, stt_s, gains_s, ew_s, ep_s, kf_s, kft_s, mi_s, tab_s, pos_s,
    ar_l, ar_r, ar_x, ar_z, ar_o,
    kf_sem, gs, gr, bs, br, cs_s, cs_r, xs, xr, zs, zr, azs, azr, axs, axr, acs, acr,
    rcs, rcr, rxs, rxr, rzs, rzr, ros, ror,
):
    nx, nl, ny, nh, nc = sizes
    x, zl, y, zh, co = (lax.axis_index(a) for a in AXES)
    devices = nx * nl * ny * nh * nc
    gy, gz = zl * ny + y, zh * nc + co
    n_gy, n_gz = nl * ny, nh * nc
    owner = ((x * nl + zl) * ny + y) * nh * nc + zh * nc + co
    norm_atoms = (ATOMS * devices) ** (-0.5)
    norm_k = (ROWS * devices) ** (-0.5)

    def brick(ox, oy, oz):
        bx = lax.rem(x + (ox + nx), nx)
        by = lax.rem(gy + (oy + n_gy), n_gy)
        bz = lax.rem(gz + (oz + n_gz), n_gz)
        return (bx, by // ny, lax.rem(by, ny), bz // nc, lax.rem(bz, nc))

    xy_steps = [(i, j) for i in range(nx) for j in range(ny) if (i, j) != (0, 0)]
    z_steps = [(i, j) for i in range(nh) for j in range(nl) if (i, j) != (0, 0)]

    def xy_to(step):
        return lax.rem(x + step[0], nx), lax.rem(y + step[1], ny)

    def z_to(step):
        return lax.rem(zh + step[0], nh), lax.rem(zl + step[1], nl)

    sibling = (x, zl, y, zh, nc - 1 - co)

    def xy_dev(step):
        tx, ty = xy_to(step)
        return (tx, zl, ty, zh, co)

    def z_dev(step):
        th, tl = z_to(step)
        return (x, tl, y, th, co)

    def send(src, dst, ssem, rsem, dev):
        copy = pltpu.make_async_remote_copy(
            src_ref=src, dst_ref=dst, send_sem=ssem, recv_sem=rsem, device_id=dev, device_id_type=MESH
        )
        copy.start()
        return copy

    kf_copy = pltpu.make_async_copy(kf_ref.at[:, pl.ds(pl.multiple_of(owner // 16 * 128, 128), 128)], kf_s, kf_sem)
    kf_copy.start()

    barrier = pltpu.get_barrier_semaphore()
    partners = [brick(*o) for o in GHOSTS] + [xy_dev(s) for s in xy_steps] + [z_dev(s) for s in z_steps] + [sibling]
    for dev in partners:
        pl.semaphore_signal(barrier, inc=1, device_id=dev, device_id_type=MESH)

    hb = h_ref[...]
    tab_s[...] = jnp.zeros((8, 128), f32)
    tab_s[0:4, 0:CH] = gain_ref[...]
    tab = jnp.transpose(tab_s[...])[0:CH]
    lab = lab_ref[...]
    gains = jnp.zeros((CH, ATOMS), f32)
    for s in range(4):
        gains = jnp.where(lab == s, tab[:, s : s + 1], gains)
    gains_s[...] = gains
    mix = mix_ref[...]
    mix_t = jnp.transpose(mix.astype(f32)).astype(bf16)
    z = jnp.transpose((dot_nn(mix_t, hb) * gains).astype(bf16).astype(f32)).reshape(32, 2, 8, CH)
    z = jnp.concatenate([z[:, 0], z[:, 1]], axis=2).astype(bf16)
    feat[...] = z[0:27].reshape(3, 3, 3, 8, 128)
    feat5[...] = z[27:32]
    p = pos_ref[:, 0, :]
    pos_s[...] = p
    lane = lax.broadcasted_iota(i32, (16, ATOMS), 1)
    in_block = (lane & 15) == lax.broadcasted_iota(i32, (16, ATOMS), 0)
    block_hot = jnp.where(
        lax.broadcasted_iota(i32, (32, ATOMS), 1) >> 4 == lax.broadcasted_iota(i32, (32, ATOMS), 0), 1.0, 0.0
    ).astype(bf16)
    spread = jnp.concatenate([jnp.where(in_block, p[d : d + 1], 0.0) for d in range(3)], axis=0)
    parts = dot_nt(jnp.concatenate(split3(spread), axis=0), block_hot)
    parts = (parts[0:48] + parts[48:96]) + parts[96:144]
    parts = jnp.transpose(jnp.concatenate([parts, jnp.zeros((80, 32), f32)], axis=0))
    pfeat[...] = parts[0:27].reshape(3, 3, 3, 1, 128)
    pfeat5[...] = parts[27:32].reshape(5, 1, 128)

    st = jnp.concatenate([hb, dy_ref[...]], axis=0)
    st_s[...] = st
    stt_s[...] = jnp.transpose(st.astype(f32)).astype(bf16)
    mil = mil_ref[...].astype(f32)
    mrows = jnp.concatenate([mil, mil, mil, jnp.zeros((7, mil.shape[1]), f32)], axis=0)
    mi_s[...] = mrows.astype(bf16)
    m9_s[...] = jnp.transpose(mrows).astype(bf16)
    absolute = jnp.concatenate(
        [
            (p[0:1] + x.astype(f32)) * (1.0 / nx),
            (p[1:2] + gy.astype(f32)) * (1.0 / n_gy),
            (p[2:3] + gz.astype(f32)) * (1.0 / n_gz),
        ],
        axis=0,
    )
    w_hi = absolute.astype(bf16).astype(f32)
    w_mid = (absolute - w_hi).astype(bf16).astype(f32)
    w_lo = (absolute - w_hi - w_mid).astype(bf16).astype(f32)
    p9_s[...] = jnp.concatenate([w_hi, w_mid, w_lo, jnp.zeros((7, ATOMS), f32)], axis=0).astype(bf16)

    chunk = 16 if devices >= 16 else devices

    def phase_step(n, _):
        at = pl.multiple_of(n * (chunk * ROWS), chunk * ROWS)
        t = dot_nn(m9_s[pl.ds(at, chunk * ROWS), :], p9_s[...])
        t = t - jnp.floor(t + 0.5)
        sq = t * t
        cosine = poly(COS, sq).reshape(chunk, ROWS, ATOMS)
        sine = (t * poly(SIN, sq)).reshape(chunk, ROWS, ATOMS)
        both = jnp.concatenate([cosine, sine], axis=1).reshape(chunk * 2 * ROWS, ATOMS).astype(bf16)
        cs[pl.ds(pl.multiple_of(n * (chunk * 2 * ROWS), chunk * 2 * ROWS), chunk * 2 * ROWS), :] = both
        part = dot_nn(both, stt_s[...])
        tot[pl.ds(n * (chunk // nc), chunk // nc)] = part.reshape(chunk // nc, nc, 16, 128)
        return 0

    lax.fori_loop(0, devices // chunk, phase_step, 0)

    pl.semaphore_wait(barrier, len(partners))
    core_copy = send(tot.at[:, nc - 1 - co], rec_a, cs_s.at[0], cs_r.at[0], sibling)

    ghost_copies = [
        send(pick(feat, o), region(o, gf, ge, gc), gs.at[n], gr.at[n], brick(-o[0], -o[1], -o[2]))
        for n, o in enumerate(GHOSTS)
    ] + [
        send(pick(pfeat, o), region(o, pgf, pge, pgc), gs.at[26 + n], gr.at[26 + n], brick(-o[0], -o[1], -o[2]))
        for n, o in enumerate(GHOSTS)
    ]

    e = idx_ref[...]
    slot, atom = e >> 9, e & 511
    block = atom >> 4
    o1 = (slot * 57) >> 9
    o2 = ((slot - 9 * o1) * 11) >> 5
    o3 = slot - 9 * o1 - 3 * o2
    c1 = (block * 57) >> 9
    c2 = ((block - 9 * c1) * 11) >> 5
    c3 = block - 9 * c1 - 3 * c2
    place = jnp.zeros_like(e)
    for o_n, c_n in ((o1, c1), (o2, c2), (o3, c3)):
        place = jnp.where(o_n == 1, place * 3 + c_n, place)
    base = jnp.zeros_like(e)
    for n, o in enumerate(SLOTS):
        base = jnp.where(slot == n, base_block(o), base)
    at_block = jnp.where(slot == 13, block, base + place)
    inner = atom & 15
    row = at_block * 8 + (inner & 7)
    upper = jnp.where(row >= 512, 1, 0)
    low = row - 512 * upper
    segment = 2 * upper + (inner >> 3)
    for j in range(NBR):
        meta[j] = jnp.concatenate(
            [v[j : j + 1] for v in (low, segment, at_block, inner, o1 - 1, o2 - 1, o3 - 1)]
            + [jnp.zeros((1, ATOMS), i32)],
            axis=0,
        )

    core_copy.wait_recv()

    def core_sum(n, _):
        part = tot[pl.ds(n * (nl * ny * nh), nl * ny * nh), co] + rec_a[pl.ds(n * (nl * ny * nh), nl * ny * nh)]
        a_bf[n] = part.astype(bf16).reshape(nl, ny, nh, 16, 128)
        return 0

    lax.fori_loop(0, nx, core_sum, 0)

    xy_copies = []
    for n, s in enumerate(xy_steps):
        tx, ty = xy_to(s)
        xy_copies.append(send(a_bf.at[tx, :, ty], rec_b.at[n], xs.at[n], xr.at[n], xy_dev(s)))

    def hot_step(n, _):
        for k in range(GROUP):
            m = meta[n * GROUP + k]
            at = slice(k * ATOMS, (k + 1) * ATOMS)
            onehot[n, :, at] = jnp.where(
                lax.broadcasted_iota(i32, (SEG, ATOMS), 0) == m[0:1], 1.0, 0.0
            ).astype(bf16)
            hotb[n, :, at] = jnp.where(
                lax.broadcasted_iota(i32, (BLOCKS, ATOMS), 0) == m[2:3], 1.0, 0.0
            ).astype(bf16)
        return 0

    lax.fori_loop(0, NBR // GROUP, hot_step, 0)

    for c in ghost_copies:
        c.wait_recv()

    table = jnp.concatenate(
        [
            feat[...].reshape(216, 128),
            feat5[...].reshape(40, 128),
            gf[...].reshape(432, 128),
            ge[...].reshape(288, 128),
            gc[...].reshape(64, 128),
        ],
        axis=0,
    ).astype(f32)
    table = jnp.concatenate(
        [
            jnp.concatenate([jnp.transpose(table[0:512]), jnp.zeros((128, SEG - 512), f32)], axis=1),
            jnp.transpose(table[512:1040]),
        ],
        axis=0,
    )
    table_s[...] = table.astype(bf16)
    xp_s[...] = jnp.zeros((BLOCKS, 128), f32)
    xp_s[0:27] = pfeat[...].reshape(27, 128)
    xp_s[27:32] = pfeat5[...].reshape(5, 128)
    xp_s[32:86] = pgf[...].reshape(54, 128)
    xp_s[86:122] = pge[...].reshape(36, 128)
    xp_s[122:130] = pgc[...].reshape(8, 128)
    ptable = jnp.concatenate(split3(jnp.transpose(xp_s[...])[0:48]), axis=0)
    rad = rad_ref[...]
    rad_hi, rad_lo = split2(rad)
    radt_hi, radt_lo = split2(jnp.transpose(rad))
    rad_fwd = jnp.concatenate([radt_hi, radt_hi, radt_lo], axis=1)
    rad_bwd = jnp.concatenate([rad_hi, rad_hi, rad_lo], axis=1)
    spacing = reach_sq / (NB - 1)
    centres = lax.broadcasted_iota(i32, (NB, ATOMS), 0).astype(f32) * spacing
    agg_s[...] = jnp.zeros((CH, ATOMS), f32)

    def forward_one(n, k):
        j = n * GROUP + k
        m = meta[j]
        seg_j = m[1:2]
        at = slice(k * ATOMS, (k + 1) * ATOMS)
        got = dot_nn(table_s[...], onehot[n, :, at])
        nz = jnp.where(
            seg_j < 2,
            jnp.where(seg_j == 0, got[0:CH], got[CH : 2 * CH]),
            jnp.where(seg_j == 2, got[2 * CH : 3 * CH], got[3 * CH : 4 * CH]),
        )
        near[j] = nz.astype(bf16)
        gotp = dot_nn(ptable, hotb[n, :, at])
        gotp = (gotp[0:48] + gotp[48:96]) + gotp[96:144]
        mine = lax.broadcasted_iota(i32, (16, ATOMS), 0) == m[3:4]
        near_pos = jnp.concatenate(
            [
                jnp.sum(jnp.where(mine, gotp[16 * d : 16 * d + 16], 0.0), axis=0, keepdims=True)
                for d in range(3)
            ],
            axis=0,
        )
        rel = (near_pos + m[4:7].astype(f32)) - pos_s[...]
        sq = rel * rel
        dist = sq[0:1] + sq[1:2] + sq[2:3]
        rel_s[j] = jnp.concatenate([rel, dist, jnp.zeros((4, ATOMS), f32)], axis=0)
        d = (dist - centres) / (2.0 * spacing)
        b = jnp.exp(-(d * d))
        basis_s[j] = b
        b_hi, b_lo = split2(b)
        fl = dot_nn(rad_fwd, jnp.concatenate([b_hi, b_lo, b_hi], axis=0))
        filt[j] = fl
        return fl * nz

    def forward_step(n, _):
        parts = [forward_one(n, k) for k in range(GROUP)]
        agg_s[...] += functools.reduce(jnp.add, parts)
        return 0

    lax.fori_loop(0, NBR // GROUP, forward_step, 0)

    v = agg_s[...] * NBR ** (-0.5)
    sig = 1.0 / (1.0 + jnp.exp(-v))
    u_s[...] = dy_ref[...].astype(f32) * (sig * (1.0 + v * (1.0 - sig))) * NBR ** (-0.5)

    grad_s[...] = jnp.zeros((SEG, 4 * CH), f32)
    gradp_s[...] = jnp.zeros((BLOCKS, 96), f32)
    ownpos_s[...] = jnp.zeros((8, ATOMS), f32)
    drad_s[...] = jnp.zeros((2 * NB, 2 * CH), f32)

    def backward_one(j, k):
        u = u_s[...]
        nz = near[j].astype(f32)
        dz = u * filt[j]
        df = u * nz
        df_hi, df_lo = split2(df)
        b = basis_s[j]
        b_hi, b_lo = split2(b)
        db = dot_nn(rad_bwd, jnp.concatenate([df_hi, df_lo, df_hi], axis=0))
        drad = dot_nt(jnp.concatenate([b_hi, b_lo], axis=0), jnp.concatenate([df_hi, df_lo], axis=0))
        r = rel_s[j]
        d = (r[3:4] - centres) / (2.0 * spacing)
        ddist = jnp.sum(db * b * d, axis=0, keepdims=True) * (-2.0 / (2.0 * spacing))
        drel = 2.0 * r[0:3] * ddist
        m = meta[j]
        seg_j = m[1:2]
        at = slice(k * ATOMS, (k + 1) * ATOMS)
        dgs[:, at] = jnp.concatenate([jnp.where(seg_j == q, dz, 0.0) for q in range(4)], axis=0).astype(bf16)
        drel_hi = drel.astype(bf16).astype(f32)
        mine = lax.broadcasted_iota(i32, (16, ATOMS), 0) == m[3:4]
        dgp[:, at] = jnp.concatenate(
            [jnp.where(mine, v[d : d + 1], 0.0) for v in (drel_hi, drel - drel_hi) for d in range(3)], axis=0
        ).astype(bf16)
        return drad, drel

    def backward_step(n, _):
        parts = [backward_one(n * GROUP + k, k) for k in range(GROUP)]
        drad_s[...] += functools.reduce(jnp.add, [p[0] for p in parts])
        ownpos_s[0:3] += functools.reduce(jnp.add, [p[1] for p in parts])
        grad_s[...] += dot_nt(onehot[n], dgs[...])
        gradp_s[...] += dot_nt(hotb[n], dgp[...])
        return 0

    half = NBR // GROUP // 2
    lax.fori_loop(0, half, backward_step, 0)

    for c in xy_copies:
        c.wait_recv()
    part = a_bf[x, :, y].astype(f32)
    for n in range(len(xy_steps)):
        part = part + rec_b[n].astype(f32)
    sum_b[...] = part

    z_copies = []
    for n, s in enumerate(z_steps):
        th, tl = z_to(s)
        z_copies.append(send(sum_b.at[tl, th], rec_c.at[n], zs.at[n], zr.at[n], z_dev(s)))

    lax.fori_loop(half, NBR // GROUP, backward_step, 0)

    grad = grad_s[...]
    grad = jnp.concatenate([grad[0:512, 0:128], grad[:, 128:256]], axis=0)
    own_s[...] = grad[0:256].reshape(32, 8, 128)
    sf[...] = grad[256:688].astype(bf16).reshape(6, 3, 3, 8, 128)
    se[...] = grad[688:976].astype(bf16).reshape(12, 3, 8, 128)
    sc[...] = grad[976:1040].astype(bf16).reshape(8, 8, 128)
    gradp = gradp_s[...]
    gradp = jnp.concatenate([gradp[:, 0:48] + gradp[:, 48:96], jnp.zeros((BLOCKS, 80), f32)], axis=1)
    ownp_s[...] = gradp[0:32].reshape(32, 1, 128)
    psf[...] = gradp[32:86].reshape(6, 3, 3, 1, 128)
    pse[...] = gradp[86:122].reshape(12, 3, 1, 128)
    psc[...] = gradp[122:130].reshape(8, 1, 128)
    back_copies = [
        send(region(o, sf, se, sc), region(o, rf, re, rc), bs.at[n], br.at[n], brick(*o))
        for n, o in enumerate(GHOSTS)
    ] + [
        send(region(o, psf, pse, psc), region(o, prf, pre, prc), bs.at[26 + n], br.at[26 + n], brick(*o))
        for n, o in enumerate(GHOSTS)
    ]

    for c in z_copies:
        c.wait_recv()
    total = sum_b[zl, zh]
    for n in range(len(z_steps)):
        total = total + rec_c[n]
    kf_copy.wait()
    kft_s[...] = jnp.transpose(kf_s[...])
    kf = kft_s[pl.ds(pl.multiple_of(lax.rem(owner, 16) * ROWS, ROWS), ROWS), :]
    struct = total[:, 0:CH] * norm_atoms
    back = total[:, CH : 2 * CH] * norm_k
    prod = struct * back
    filter_out[...] = prod[0:ROWS] + prod[ROWS : 2 * ROWS]
    kf2 = jnp.concatenate([kf, kf], axis=0)
    coeffs = jnp.concatenate([norm_atoms * kf2 * back, norm_k * kf2 * struct], axis=1).astype(bf16)
    g1[zl, zh] = coeffs
    az_copies = [
        send(g1.at[zl, zh], g1.at[zl, zh], azs.at[n], azr.at[n], z_dev(s)) for n, s in enumerate(z_steps)
    ]

    for c in az_copies:
        c.wait_recv()
    arr[x, :, y, :, co] = g1[...]
    ax_copies = [
        send(g1, arr.at[x, :, y, :, co], axs.at[n], axr.at[n], xy_dev(s)) for n, s in enumerate(xy_steps)
    ]

    for c in back_copies:
        c.wait_recv()
    for o in GHOSTS:
        got = region(o, rf, re, rc)[...].astype(f32)
        view = [range(3) if c == 0 else [1 - c] for c in o]
        got = got.reshape(-1, 8, 128)
        gotp = region(o, prf, pre, prc)[...].reshape(-1, 1, 128)
        n = 0
        for i in view[0]:
            for k in view[1]:
                for l in view[2]:
                    own_s[9 * i + 3 * k + l] += got[n]
                    ownp_s[9 * i + 3 * k + l] += gotp[n]
                    n += 1
    own = own_s[...]
    own = jnp.concatenate([own[:, None, :, 0:CH], own[:, None, :, CH : 2 * CH]], axis=1)
    own = jnp.transpose(own.reshape(ATOMS, CH))
    ownp = jnp.transpose(ownp_s[...].reshape(32, 128))[0:48]
    wide = dot_nn(jnp.concatenate(split3(ownp), axis=1), jnp.concatenate([block_hot] * 3, axis=0))
    ownp = jnp.concatenate(
        [
            jnp.sum(jnp.where(in_block, wide[16 * d : 16 * d + 16], 0.0), axis=0, keepdims=True)
            for d in range(3)
        ],
        axis=0,
    )
    gains = gains_s[...]
    zscaled = (own * gains).astype(bf16)
    pos_short = ownp - ownpos_s[0:3]
    ew_s[...] = dy_ref[...].astype(f32) + dot_nn(mix_ref[...], zscaled)
    weight = dot_nt(h_ref[...], zscaled)
    dr = drad_s[...]
    dr = dr[0:NB, 0:CH] + (dr[NB : 2 * NB, 0:CH] + dr[0:NB, CH : 2 * CH]) + dr[NB : 2 * NB, CH : 2 * CH]
    small = jnp.concatenate(
        [
            jnp.concatenate([weight[0:32], weight[32:64]], axis=1),
            jnp.concatenate([dr[0:8], dr[8:16]], axis=1),
            jnp.zeros((8, 128), f32),
        ],
        axis=0,
    )
    ar_l[...] = small.reshape(2, 24, 128)
    rc_copy = send(ar_l.at[nc - 1 - co], ar_r, rcs.at[0], rcr.at[0], sibling)

    rc_copy.wait_recv()
    ar_x[x * ny + y] = ar_l[co] + ar_r[...]
    rx_copies = [
        send(ar_x.at[x * ny + y], ar_x.at[x * ny + y], rxs.at[n], rxr.at[n], xy_dev(s))
        for n, s in enumerate(xy_steps)
    ]

    for c in ax_copies:
        c.wait_recv()
    ac_copy = send(
        arr.at[:, :, :, :, co], arr.at[:, :, :, :, co], acs.at[0], acr.at[0], sibling
    )
    for c in rx_copies:
        c.wait_recv()
    part = ar_x[0]
    for n in range(1, nx * ny):
        part = part + ar_x[n]
    ar_z[zl * nh + zh] = part
    rz_copies = [
        send(ar_z.at[zl * nh + zh], ar_z.at[zl * nh + zh], rzs.at[n], rzr.at[n], z_dev(s))
        for n, s in enumerate(z_steps)
    ]
    ac_copy.wait_recv()

    ep_s[...] = jnp.zeros((16, ATOMS), f32)

    def ewald_step(n, _):
        rows_n = chunk * 2 * ROWS
        co_n = arr_chunk(n)
        cs_n = cs[pl.ds(pl.multiple_of(n * rows_n, rows_n), rows_n), :]
        along = dot_nn(co_n, st_s[...]).reshape(chunk, 2, ROWS, ATOMS)
        trig = cs_n.astype(f32).reshape(chunk, 2, ROWS, ATOMS)
        ag = (along[:, 1] * trig[:, 0] - along[:, 0] * trig[:, 1]).reshape(chunk * ROWS, ATOMS)
        ag_hi, ag_lo = split2(ag)
        m_n = mi_s[:, pl.ds(pl.multiple_of(n * (chunk * ROWS), chunk * ROWS), chunk * ROWS)]
        ep_s[...] += dot_nn(m_n, ag_hi) + dot_nn(m_n, ag_lo)
        co_t = jnp.transpose(co_n.astype(f32))[0:CH].astype(bf16)
        ew_s[...] += dot_nn(co_t, cs_n)
        return 0

    per_x = nl * ny * nh * nc // chunk

    def arr_chunk(n):
        i = n // per_x
        r = lax.rem(n, per_x)
        if nl * ny * nh * nc // nl == chunk:
            return arr[i, r].reshape(chunk * 16, 128)
        return arr[i].reshape(chunk * 16, 128)

    steps = devices // chunk
    lax.fori_loop(0, steps, ewald_step, 0)
    atom_out[...] = ew_s[...].astype(bf16)
    ep = ep_s[0:3]
    turn = 2.0 * math.pi
    pos_out[:, 0, :] = pos_short + jnp.concatenate(
        [ep[0:1] * (turn / nx), ep[1:2] * (turn / n_gy), ep[2:3] * (turn / n_gz)], axis=0
    )

    for c in rz_copies:
        c.wait_recv()
    part = ar_z[0]
    for n in range(1, nl * nh):
        part = part + ar_z[n]
    ar_o[co] = part
    ro_copy = send(ar_o.at[co], ar_o.at[co], ros.at[0], ror.at[0], sibling)
    ro_copy.wait_recv()
    full = ar_o[...].reshape(48, 128)
    weight_out[...] = jnp.concatenate([full[0:32, 0:CH], full[0:32, CH : 2 * CH]], axis=0)
    radial_out[...] = jnp.concatenate([full[32:40, 0:CH], full[32:40, CH : 2 * CH]], axis=0)

    for c in (
        ghost_copies + [core_copy] + xy_copies + z_copies + az_copies + ax_copies + back_copies
        + [rc_copy, ac_copy] + rx_copies + rz_copies + [ro_copy]
    ):
        c.wait_send()


def deliver_kernel(*refs):
    n = (len(refs) - 1) // 3
    copies = [pltpu.make_async_copy(refs[i], refs[2 * n + i], refs[-1].at[i]) for i in range(n)]
    for c in copies:
        c.start()
    for c in copies:
        c.wait()
    for i in range(n):
        refs[n + i][...] = refs[2 * n + i][...]


def deliver(arrays):
    return pl.pallas_call(
        deliver_kernel,
        out_shape=tuple(jax.ShapeDtypeStruct(a.shape, a.dtype) for a in arrays),
        in_specs=[pl.BlockSpec(memory_space=pl.ANY)] * len(arrays),
        out_specs=(pl.BlockSpec(memory_space=pltpu.VMEM),) * len(arrays),
        scratch_shapes=[pltpu.VMEM(a.shape, a.dtype) for a in arrays]
        + [pltpu.SemaphoreType.DMA((len(arrays),))],
        compiler_params=pltpu.CompilerParams(vmem_limit_bytes=62 * 1024 * 1024),
        name="deliver",
    )(*arrays)


def shards(sizes, h, dy, pos, labels, entries, miller, kfilter, mix, table, radial):
    nx, nl, ny, nh, nc = sizes
    devices = nx * nl * ny * nh * nc
    k = ROWS * devices
    nxy, nz = nx * ny, nl * nh
    vmem = pl.BlockSpec(memory_space=pltpu.VMEM)
    dma = pltpu.SemaphoreType.DMA
    plane = devices // nc
    scratch = [
        pltpu.VMEM((2 * k, ATOMS), bf16),
        pltpu.VMEM((plane, nc, 16, 128), f32),
        pltpu.VMEM((nx, nl, ny, nh, nc, 16, 128), bf16),
        pltpu.VMEM((3, 3, 3, 8, 128), bf16),
        pltpu.VMEM((5, 8, 128), bf16),
        pltpu.VMEM((6, 3, 3, 8, 128), bf16),
        pltpu.VMEM((12, 3, 8, 128), bf16),
        pltpu.VMEM((8, 8, 128), bf16),
        pltpu.VMEM((3, 3, 3, 1, 128), f32),
        pltpu.VMEM((5, 1, 128), f32),
    ]
    for _ in range(3):
        scratch += [
            pltpu.VMEM((6, 3, 3, 1, 128), f32),
            pltpu.VMEM((12, 3, 1, 128), f32),
            pltpu.VMEM((8, 1, 128), f32),
        ]
    scratch += [
        pltpu.VMEM((4 * CH, SEG), bf16),
        pltpu.VMEM((BLOCKS, 128), f32),
        pltpu.VMEM((NBR // GROUP, BLOCKS, GROUP * ATOMS), bf16),
        pltpu.VMEM((96, GROUP * ATOMS), bf16),
        pltpu.VMEM((BLOCKS, 96), f32),
        pltpu.VMEM((32, 1, 128), f32),
        pltpu.VMEM((NBR, 8, ATOMS), i32),
        pltpu.VMEM((NBR // GROUP, SEG, GROUP * ATOMS), bf16),
        pltpu.VMEM((NBR, CH, ATOMS), bf16),
        pltpu.VMEM((NBR, CH, ATOMS), f32),
        pltpu.VMEM((NBR, NB, ATOMS), f32),
        pltpu.VMEM((NBR, 8, ATOMS), f32),
        pltpu.VMEM((4 * CH, GROUP * ATOMS), bf16),
        pltpu.VMEM((CH, ATOMS), f32),
        pltpu.VMEM((SEG, 4 * CH), f32),
        pltpu.VMEM((32, 8, 128), f32),
        pltpu.VMEM((8, ATOMS), f32),
        pltpu.VMEM((CH, ATOMS), f32),
        pltpu.VMEM((2 * NB, 2 * CH), f32),
        pltpu.VMEM((6, 3, 3, 8, 128), bf16),
        pltpu.VMEM((12, 3, 8, 128), bf16),
        pltpu.VMEM((8, 8, 128), bf16),
        pltpu.VMEM((6, 3, 3, 8, 128), bf16),
        pltpu.VMEM((12, 3, 8, 128), bf16),
        pltpu.VMEM((8, 8, 128), bf16),
        pltpu.VMEM((plane, 16, 128), f32),
        pltpu.VMEM((nx, nl, ny, nh, 16, 128), bf16),
        pltpu.VMEM((nxy - 1, nl, nh, 16, 128), bf16),
        pltpu.VMEM((nl, nh, 16, 128), f32),
        pltpu.VMEM((nz - 1, 16, 128), f32),
        pltpu.VMEM((nl, nh, 16, 128), bf16),
        pltpu.VMEM((k, 16), bf16),
        pltpu.VMEM((16, ATOMS), bf16),
        pltpu.VMEM((2 * CH, ATOMS), bf16),
        pltpu.VMEM((ATOMS, 2 * CH), bf16),
        pltpu.VMEM((CH, ATOMS), f32),
        pltpu.VMEM((CH, ATOMS), f32),
        pltpu.VMEM((16, ATOMS), f32),
        pltpu.VMEM((CH, 128), f32),
        pltpu.VMEM((128, CH), f32),
        pltpu.VMEM((16, k), bf16),
        pltpu.VMEM((8, 128), f32),
        pltpu.VMEM((3, ATOMS), f32),
        pltpu.VMEM((2, 24, 128), f32),
        pltpu.VMEM((24, 128), f32),
        pltpu.VMEM((nxy, 24, 128), f32),
        pltpu.VMEM((nz, 24, 128), f32),
        pltpu.VMEM((2, 24, 128), f32),
        dma,
    ]
    for count in (52, 52, 1, nxy - 1, nz - 1, nz - 1, nxy - 1, 1, 1, nxy - 1, nz - 1, 1):
        scratch += [dma((count,)), dma((count,))]
    out = pl.pallas_call(
        functools.partial(kernel, sizes),
        out_shape=(
            jax.ShapeDtypeStruct((CH, ATOMS), bf16),
            jax.ShapeDtypeStruct((3, 1, ATOMS), f32),
            jax.ShapeDtypeStruct((CH, CH), f32),
            jax.ShapeDtypeStruct((NB, CH), f32),
            jax.ShapeDtypeStruct((ROWS, CH), f32),
        ),
        in_specs=[vmem] * 6 + [pl.BlockSpec(memory_space=pl.ANY)] + [vmem] * 3,
        out_specs=(vmem,) * 5,
        scratch_shapes=scratch,
        compiler_params=pltpu.CompilerParams(
            collective_id=0, has_side_effects=True, vmem_limit_bytes=62 * 1024 * 1024
        ),
        name="layer",
    )(
        h[0, 0, 0], dy[0, 0, 0], jnp.transpose(pos, (0, 1, 3, 2, 4))[0, 0], labels[0, 0], entries[0, 0, 0],
        miller, kfilter.T, mix, table, radial,
    )
    out = deliver(out)
    return (out[0][None, None, None], jnp.transpose(out[1][None, None], (0, 1, 3, 2, 4)), out[2], out[3], out[4])


def solution(mesh):
    sizes = (mesh.shape["gx"], 4, mesh.shape["gy"] // 4, mesh.shape["gz"] // 2, 2)
    finer = Mesh(mesh.devices.reshape(sizes), AXES)
    brick = P("gx", GY, GZ, None, None)
    return jax.shard_map(
        functools.partial(shards, sizes),
        mesh=finer,
        in_specs=(brick, brick, brick, P("gx", GY, GZ, None), brick, P(), P(), P(), P(), P()),
        out_specs=(brick, brick, P(), P(), P(AXES, None)),
        check_vma=False,
    )
```

```python
import functools
import math

import jax
import jax.numpy as jnp
from jax import lax
from jax.experimental import pallas as pl
from jax.experimental.pallas import tpu as pltpu
from jax.sharding import Mesh
from jax.sharding import PartitionSpec as P

AXES = ("gx", "gy_0", "gy_1", "gz_0", "gz_1")
GY = ("gy_0", "gy_1")
GZ = ("gz_0", "gz_1")
MESH = pl.DeviceIdType.MESH
f32, bf16, i32 = jnp.float32, jnp.bfloat16, jnp.int32

CH = 64
ATOMS = 512
NBR = 16
NB = 16
ROWS = 8
SEG = 528
BLOCKS = 144
EWALD = 4
GROUP = 8
reach_sq = 0.75

COS = (
    0.9999999890590228,
    -19.739204499454026,
    64.93911745990036,
    -85.45013953095037,
    60.16763095136588,
    -25.96759924965491,
    6.528658162567069,
)
SIN = (
    6.283185302511503,
    -41.34170040531769,
    81.60513138580204,
    -76.7030153539128,
    42.02592698618416,
    -14.899846668691637,
    3.238137510515757,
)

SLOTS = [(ox, oy, oz) for ox in (-1, 0, 1) for oy in (-1, 0, 1) for oz in (-1, 0, 1)]
FACES = [o for o in SLOTS if sum(map(abs, o)) == 1]
EDGES = [o for o in SLOTS if sum(map(abs, o)) == 2]
CORNERS = [o for o in SLOTS if sum(map(abs, o)) == 3]
GHOSTS = FACES + EDGES + CORNERS


def base_block(o):
    if o in FACES:
        return 32 + 9 * FACES.index(o)
    if o in EDGES:
        return 32 + 54 + 3 * EDGES.index(o)
    if o in CORNERS:
        return 32 + 54 + 36 + CORNERS.index(o)
    return 0


def poly(coef, x):
    acc = jnp.full_like(x, coef[-1])
    for c in coef[-2::-1]:
        acc = acc * x + c
    return acc


def split2(x):
    hi = x.astype(bf16)
    return hi, (x - hi.astype(f32)).astype(bf16)


def split3(x):
    hi = x.astype(bf16)
    rest = x - hi.astype(f32)
    mid = rest.astype(bf16)
    return hi, mid, (rest - mid.astype(f32)).astype(bf16)


def dot_nn(a, b):
    return jnp.dot(a, b, preferred_element_type=f32)


def dot_nt(a, b):
    return lax.dot_general(a, b, (((1,), (1,)), ((), ())), preferred_element_type=f32)


def pick(ref, o):
    return ref.at[tuple(slice(None) if c == 0 else 1 - c for c in o)]


def region(o, faces, edges, corners):
    if o in FACES:
        return faces.at[FACES.index(o)]
    if o in EDGES:
        return edges.at[EDGES.index(o)]
    return corners.at[CORNERS.index(o)]


def kernel(
    sizes,
    h_in, dy_in, pos_in, lab_in, idx_in, mil_in, kf_ref, mix_in, gain_in, rad_in,
    atom_out, pos_out, weight_out, radial_out, filter_out,
    cs, tot, arr,
    feat, feat5, gf, ge, gc,
    pfeat, pfeat5, pgf, pge, pgc, psf, pse, psc, prf, pre, prc, table_s, xp_s, hotb, dgp, gradp_s, ownp_s,
    meta, onehot, near, filt, basis_s, rel_s, dgs, agg_s, grad_s, own_s, ownpos_s, u_s, drad_s,
    sf, se, sc, rf, re, rc,
    rec_a, a_bf, rec_b, sum_b, rec_c, g1,
    m9_s, p9_s, st_s, stt_s, gains_s, ew_s, ep_s, kf_s, kft_s, mi_s, tab_s, pos_s,
    ar_l, ar_r, ar_x, ar_z, ar_o,
    h_ref, dy_ref, pos_ref, lab_ref, idx_ref, mil_ref, mix_ref, gain_ref, rad_ref, in_sem,
    kf_sem, gs, gr, bs, br, cs_s, cs_r, xs, xr, zs, zr, azs, azr, axs, axr, acs, acr,
    rcs, rcr, rxs, rxr, rzs, rzr, ros, ror,
):
    nx, nl, ny, nh, nc = sizes
    x, zl, y, zh, co = (lax.axis_index(a) for a in AXES)
    devices = nx * nl * ny * nh * nc
    gy, gz = zl * ny + y, zh * nc + co
    n_gy, n_gz = nl * ny, nh * nc
    owner = ((x * nl + zl) * ny + y) * nh * nc + zh * nc + co
    norm_atoms = (ATOMS * devices) ** (-0.5)
    norm_k = (ROWS * devices) ** (-0.5)

    def brick(ox, oy, oz):
        bx = lax.rem(x + (ox + nx), nx)
        by = lax.rem(gy + (oy + n_gy), n_gy)
        bz = lax.rem(gz + (oz + n_gz), n_gz)
        return (bx, by // ny, lax.rem(by, ny), bz // nc, lax.rem(bz, nc))

    xy_steps = [(i, j) for i in range(nx) for j in range(ny) if (i, j) != (0, 0)]
    z_steps = [(i, j) for i in range(nh) for j in range(nl) if (i, j) != (0, 0)]

    def xy_to(step):
        return lax.rem(x + step[0], nx), lax.rem(y + step[1], ny)

    def z_to(step):
        return lax.rem(zh + step[0], nh), lax.rem(zl + step[1], nl)

    sibling = (x, zl, y, zh, nc - 1 - co)

    def xy_dev(step):
        tx, ty = xy_to(step)
        return (tx, zl, ty, zh, co)

    def z_dev(step):
        th, tl = z_to(step)
        return (x, tl, y, th, co)

    def send(src, dst, ssem, rsem, dev):
        copy = pltpu.make_async_remote_copy(
            src_ref=src, dst_ref=dst, send_sem=ssem, recv_sem=rsem, device_id=dev, device_id_type=MESH
        )
        copy.start()
        return copy

    in_copies = [
        pltpu.make_async_copy(a, b, in_sem.at[n])
        for n, (a, b) in enumerate(
            (
                (h_in, h_ref), (pos_in, pos_ref), (lab_in, lab_ref), (mix_in, mix_ref), (gain_in, gain_ref),
                (mil_in, mil_ref), (dy_in, dy_ref), (idx_in, idx_ref), (rad_in, rad_ref),
            )
        )
    ]
    for c in in_copies:
        c.start()
    kf_copy = pltpu.make_async_copy(kf_ref.at[:, pl.ds(pl.multiple_of(owner // 16 * 128, 128), 128)], kf_s, kf_sem)
    kf_copy.start()

    barrier = pltpu.get_barrier_semaphore()
    partners = [brick(*o) for o in GHOSTS] + [xy_dev(s) for s in xy_steps] + [z_dev(s) for s in z_steps] + [sibling]
    for dev in partners:
        pl.semaphore_signal(barrier, inc=1, device_id=dev, device_id_type=MESH)

    for c in in_copies:
        c.wait()

    hb = h_ref[...]
    tab_s[...] = jnp.zeros((8, 128), f32)
    tab_s[0:4, 0:CH] = gain_ref[...]
    tab = jnp.transpose(tab_s[...])[0:CH]
    lab = lab_ref[...]
    gains = jnp.zeros((CH, ATOMS), f32)
    for s in range(4):
        gains = jnp.where(lab == s, tab[:, s : s + 1], gains)
    gains_s[...] = gains
    mix = mix_ref[...]
    mix_t = jnp.transpose(mix.astype(f32)).astype(bf16)
    z = jnp.transpose((dot_nn(mix_t, hb) * gains).astype(bf16).astype(f32)).reshape(32, 2, 8, CH)
    z = jnp.concatenate([z[:, 0], z[:, 1]], axis=2).astype(bf16)
    feat[...] = z[0:27].reshape(3, 3, 3, 8, 128)
    feat5[...] = z[27:32]
    p = pos_ref[:, 0, :]
    pos_s[...] = p
    lane = lax.broadcasted_iota(i32, (16, ATOMS), 1)
    in_block = (lane & 15) == lax.broadcasted_iota(i32, (16, ATOMS), 0)
    block_hot = jnp.where(
        lax.broadcasted_iota(i32, (32, ATOMS), 1) >> 4 == lax.broadcasted_iota(i32, (32, ATOMS), 0), 1.0, 0.0
    ).astype(bf16)
    spread = jnp.concatenate([jnp.where(in_block, p[d : d + 1], 0.0) for d in range(3)], axis=0)
    parts = dot_nt(jnp.concatenate(split3(spread), axis=0), block_hot)
    parts = (parts[0:48] + parts[48:96]) + parts[96:144]
    parts = jnp.transpose(jnp.concatenate([parts, jnp.zeros((80, 32), f32)], axis=0))
    pfeat[...] = parts[0:27].reshape(3, 3, 3, 1, 128)
    pfeat5[...] = parts[27:32].reshape(5, 1, 128)

    st = jnp.concatenate([hb, dy_ref[...]], axis=0)
    st_s[...] = st
    stt_s[...] = jnp.transpose(st.astype(f32)).astype(bf16)
    mil = mil_ref[...].astype(f32)
    mrows = jnp.concatenate([mil, mil, mil, jnp.zeros((7, mil.shape[1]), f32)], axis=0)
    mrows = jnp.transpose(mrows).reshape(devices // nc, nc, ROWS, 16)
    mrows = jnp.concatenate([mrows[:, c] for c in range(nc)], axis=0).reshape(devices * ROWS, 16)
    m9_s[...] = mrows.astype(bf16)
    mi_s[...] = jnp.transpose(mrows).astype(bf16)
    absolute = jnp.concatenate(
        [
            (p[0:1] + x.astype(f32)) * (1.0 / nx),
            (p[1:2] + gy.astype(f32)) * (1.0 / n_gy),
            (p[2:3] + gz.astype(f32)) * (1.0 / n_gz),
        ],
        axis=0,
    )
    w_hi = absolute.astype(bf16).astype(f32)
    w_mid = (absolute - w_hi).astype(bf16).astype(f32)
    w_lo = (absolute - w_hi - w_mid).astype(bf16).astype(f32)
    p9_s[...] = jnp.concatenate([w_hi, w_mid, w_lo, jnp.zeros((7, ATOMS), f32)], axis=0).astype(bf16)

    chunk = 16
    per_core = devices // nc // chunk

    def phase_step(n, _):
        at = pl.multiple_of(n * (chunk * ROWS), chunk * ROWS)
        t = dot_nn(m9_s[pl.ds(at, chunk * ROWS), :], p9_s[...])
        t = t - jnp.floor(t + 0.5)
        sq = t * t
        cosine = poly(COS, sq).reshape(chunk, ROWS, ATOMS)
        sine = (t * poly(SIN, sq)).reshape(chunk, ROWS, ATOMS)
        both = jnp.concatenate([cosine, sine], axis=1).reshape(chunk * 2 * ROWS, ATOMS).astype(bf16)
        cs[pl.ds(pl.multiple_of(n * (chunk * 2 * ROWS), chunk * 2 * ROWS), chunk * 2 * ROWS), :] = both
        part = dot_nn(both, stt_s[...])
        tot[n // per_core, pl.ds(lax.rem(n, per_core) * chunk, chunk)] = part.reshape(chunk, 16, 128)
        return 0

    lax.fori_loop(0, devices // chunk, phase_step, 0)

    pl.semaphore_wait(barrier, len(partners))
    core_copy = send(tot.at[nc - 1 - co], rec_a, cs_s.at[0], cs_r.at[0], sibling)

    ghost_copies = [
        send(pick(feat, o), region(o, gf, ge, gc), gs.at[n], gr.at[n], brick(-o[0], -o[1], -o[2]))
        for n, o in enumerate(GHOSTS)
    ] + [
        send(pick(pfeat, o), region(o, pgf, pge, pgc), gs.at[26 + n], gr.at[26 + n], brick(-o[0], -o[1], -o[2]))
        for n, o in enumerate(GHOSTS)
    ]

    e = idx_ref[...]
    slot, atom = e >> 9, e & 511
    block = atom >> 4
    o1 = (slot * 57) >> 9
    o2 = ((slot - 9 * o1) * 11) >> 5
    o3 = slot - 9 * o1 - 3 * o2
    c1 = (block * 57) >> 9
    c2 = ((block - 9 * c1) * 11) >> 5
    c3 = block - 9 * c1 - 3 * c2
    place = jnp.zeros_like(e)
    for o_n, c_n in ((o1, c1), (o2, c2), (o3, c3)):
        place = jnp.where(o_n == 1, place * 3 + c_n, place)
    base = jnp.zeros_like(e)
    for n, o in enumerate(SLOTS):
        base = jnp.where(slot == n, base_block(o), base)
    at_block = jnp.where(slot == 13, block, base + place)
    inner = atom & 15
    row = at_block * 8 + (inner & 7)
    upper = jnp.where(row >= 512, 1, 0)
    low = row - 512 * upper
    segment = 2 * upper + (inner >> 3)
    for j in range(NBR):
        meta[j] = jnp.concatenate(
            [v[j : j + 1] for v in (low, segment, at_block, inner, o1 - 1, o2 - 1, o3 - 1)]
            + [jnp.zeros((1, ATOMS), i32)],
            axis=0,
        )

    core_copy.wait_recv()

    def core_sum(n, _):
        part = tot[co, pl.ds(n * (nl * ny * nh), nl * ny * nh)] + rec_a[pl.ds(n * (nl * ny * nh), nl * ny * nh)]
        a_bf[n] = part.astype(bf16).reshape(nl, ny, nh, 16, 128)
        return 0

    lax.fori_loop(0, nx, core_sum, 0)

    xy_copies = []
    for n, s in enumerate(xy_steps):
        tx, ty = xy_to(s)
        xy_copies.append(send(a_bf.at[tx, :, ty], rec_b.at[n], xs.at[n], xr.at[n], xy_dev(s)))

    def hot_step(n, _):
        for k in range(GROUP):
            m = meta[n * GROUP + k]
            at = slice(k * ATOMS, (k + 1) * ATOMS)
            onehot[n, :, at] = jnp.where(
                lax.broadcasted_iota(i32, (SEG, ATOMS), 0) == m[0:1], 1.0, 0.0
            ).astype(bf16)
            hotb[n, :, at] = jnp.where(
                lax.broadcasted_iota(i32, (BLOCKS, ATOMS), 0) == m[2:3], 1.0, 0.0
            ).astype(bf16)
        return 0

    lax.fori_loop(0, NBR // GROUP, hot_step, 0)

    for c in ghost_copies:
        c.wait_recv()

    table = jnp.concatenate(
        [
            feat[...].reshape(216, 128),
            feat5[...].reshape(40, 128),
            gf[...].reshape(432, 128),
            ge[...].reshape(288, 128),
            gc[...].reshape(64, 128),
        ],
        axis=0,
    ).astype(f32)
    table = jnp.concatenate(
        [
            jnp.concatenate([jnp.transpose(table[0:512]), jnp.zeros((128, SEG - 512), f32)], axis=1),
            jnp.transpose(table[512:1040]),
        ],
        axis=0,
    )
    table_s[...] = table.astype(bf16)
    xp_s[...] = jnp.zeros((BLOCKS, 128), f32)
    xp_s[0:27] = pfeat[...].reshape(27, 128)
    xp_s[27:32] = pfeat5[...].reshape(5, 128)
    xp_s[32:86] = pgf[...].reshape(54, 128)
    xp_s[86:122] = pge[...].reshape(36, 128)
    xp_s[122:130] = pgc[...].reshape(8, 128)
    ptable = jnp.concatenate(split3(jnp.transpose(xp_s[...])[0:48]), axis=0)
    rad = rad_ref[...]
    rad_hi, rad_lo = split2(rad)
    radt_hi, radt_lo = split2(jnp.transpose(rad))
    rad_fwd = jnp.concatenate([radt_hi, radt_hi, radt_lo], axis=1)
    rad_bwd = jnp.concatenate([rad_hi, rad_hi, rad_lo], axis=1)
    spacing = reach_sq / (NB - 1)
    centres = lax.broadcasted_iota(i32, (NB, ATOMS), 0).astype(f32) * spacing
    agg_s[...] = jnp.zeros((CH, ATOMS), f32)

    def forward_one(n, k):
        j = n * GROUP + k
        m = meta[j]
        seg_j = m[1:2]
        at = slice(k * ATOMS, (k + 1) * ATOMS)
        got = dot_nn(table_s[...], onehot[n, :, at])
        nz = jnp.where(
            seg_j < 2,
            jnp.where(seg_j == 0, got[0:CH], got[CH : 2 * CH]),
            jnp.where(seg_j == 2, got[2 * CH : 3 * CH], got[3 * CH : 4 * CH]),
        )
        near[j] = nz.astype(bf16)
        gotp = dot_nn(ptable, hotb[n, :, at])
        gotp = (gotp[0:48] + gotp[48:96]) + gotp[96:144]
        mine = lax.broadcasted_iota(i32, (16, ATOMS), 0) == m[3:4]
        near_pos = jnp.concatenate(
            [
                jnp.sum(jnp.where(mine, gotp[16 * d : 16 * d + 16], 0.0), axis=0, keepdims=True)
                for d in range(3)
            ],
            axis=0,
        )
        rel = (near_pos + m[4:7].astype(f32)) - pos_s[...]
        sq = rel * rel
        dist = sq[0:1] + sq[1:2] + sq[2:3]
        rel_s[j] = jnp.concatenate([rel, dist, jnp.zeros((4, ATOMS), f32)], axis=0)
        d = (dist - centres) / (2.0 * spacing)
        b = jnp.exp(-(d * d))
        basis_s[j] = b
        b_hi, b_lo = split2(b)
        fl = dot_nn(rad_fwd, jnp.concatenate([b_hi, b_lo, b_hi], axis=0))
        filt[j] = fl
        return fl * nz

    def forward_step(n, _):
        parts = [forward_one(n, k) for k in range(GROUP)]
        agg_s[...] += functools.reduce(jnp.add, parts)
        return 0

    half = NBR // GROUP // 2
    lax.fori_loop(0, half, forward_step, 0)

    for c in xy_copies:
        c.wait_recv()
    part = a_bf[x, :, y].astype(f32)
    for n in range(len(xy_steps)):
        part = part + rec_b[n].astype(f32)
    sum_b[...] = part

    z_copies = []
    for n, s in enumerate(z_steps):
        th, tl = z_to(s)
        z_copies.append(send(sum_b.at[tl, th], rec_c.at[n], zs.at[n], zr.at[n], z_dev(s)))

    lax.fori_loop(half, NBR // GROUP, forward_step, 0)

    v = agg_s[...] * NBR ** (-0.5)
    sig = 1.0 / (1.0 + jnp.exp(-v))
    u_s[...] = dy_ref[...].astype(f32) * (sig * (1.0 + v * (1.0 - sig))) * NBR ** (-0.5)

    grad_s[...] = jnp.zeros((SEG, 4 * CH), f32)
    gradp_s[...] = jnp.zeros((BLOCKS, 96), f32)
    ownpos_s[...] = jnp.zeros((8, ATOMS), f32)
    drad_s[...] = jnp.zeros((2 * NB, 2 * CH), f32)

    def backward_one(j, k):
        u = u_s[...]
        nz = near[j].astype(f32)
        dz = u * filt[j]
        df = u * nz
        df_hi, df_lo = split2(df)
        b = basis_s[j]
        b_hi, b_lo = split2(b)
        db = dot_nn(rad_bwd, jnp.concatenate([df_hi, df_lo, df_hi], axis=0))
        drad = dot_nt(jnp.concatenate([b_hi, b_lo], axis=0), jnp.concatenate([df_hi, df_lo], axis=0))
        r = rel_s[j]
        d = (r[3:4] - centres) / (2.0 * spacing)
        ddist = jnp.sum(db * b * d, axis=0, keepdims=True) * (-2.0 / (2.0 * spacing))
        drel = 2.0 * r[0:3] * ddist
        m = meta[j]
        seg_j = m[1:2]
        at = slice(k * ATOMS, (k + 1) * ATOMS)
        dgs[:, at] = jnp.concatenate([jnp.where(seg_j == q, dz, 0.0) for q in range(4)], axis=0).astype(bf16)
        drel_hi = drel.astype(bf16).astype(f32)
        mine = lax.broadcasted_iota(i32, (16, ATOMS), 0) == m[3:4]
        dgp[:, at] = jnp.concatenate(
            [jnp.where(mine, v[d : d + 1], 0.0) for v in (drel_hi, drel - drel_hi) for d in range(3)], axis=0
        ).astype(bf16)
        return drad, drel

    def backward_step(n, _):
        parts = [backward_one(n * GROUP + k, k) for k in range(GROUP)]
        drad_s[...] += functools.reduce(jnp.add, [p[0] for p in parts])
        ownpos_s[0:3] += functools.reduce(jnp.add, [p[1] for p in parts])
        grad_s[...] += dot_nt(onehot[n], dgs[...])
        gradp_s[...] += dot_nt(hotb[n], dgp[...])
        return 0

    lax.fori_loop(0, half, backward_step, 0)

    for c in z_copies:
        c.wait_recv()
    total = sum_b[zl, zh]
    for n in range(len(z_steps)):
        total = total + rec_c[n]
    kf_copy.wait()
    kft_s[...] = jnp.transpose(kf_s[...])
    kf = kft_s[pl.ds(pl.multiple_of(lax.rem(owner, 16) * ROWS, ROWS), ROWS), :]
    struct = total[:, 0:CH] * norm_atoms
    back = total[:, CH : 2 * CH] * norm_k
    prod = struct * back
    filter_out[...] = prod[0:ROWS] + prod[ROWS : 2 * ROWS]
    kf2 = jnp.concatenate([kf, kf], axis=0)
    coeffs = jnp.concatenate([norm_atoms * kf2 * back, norm_k * kf2 * struct], axis=1).astype(bf16)
    g1[zl, zh] = coeffs
    az_copies = [
        send(g1.at[zl, zh], g1.at[zl, zh], azs.at[n], azr.at[n], z_dev(s)) for n, s in enumerate(z_steps)
    ]

    lax.fori_loop(half, NBR // GROUP, backward_step, 0)

    grad = grad_s[...]
    grad = jnp.concatenate([grad[0:512, 0:128], grad[:, 128:256]], axis=0)
    own_s[...] = grad[0:256].reshape(32, 8, 128)
    sf[...] = grad[256:688].astype(bf16).reshape(6, 3, 3, 8, 128)
    se[...] = grad[688:976].astype(bf16).reshape(12, 3, 8, 128)
    sc[...] = grad[976:1040].astype(bf16).reshape(8, 8, 128)
    gradp = gradp_s[...]
    gradp = jnp.concatenate([gradp[:, 0:48] + gradp[:, 48:96], jnp.zeros((BLOCKS, 80), f32)], axis=1)
    ownp_s[...] = gradp[0:32].reshape(32, 1, 128)
    psf[...] = gradp[32:86].reshape(6, 3, 3, 1, 128)
    pse[...] = gradp[86:122].reshape(12, 3, 1, 128)
    psc[...] = gradp[122:130].reshape(8, 1, 128)
    back_copies = [
        send(region(o, sf, se, sc), region(o, rf, re, rc), bs.at[n], br.at[n], brick(*o))
        for n, o in enumerate(GHOSTS)
    ] + [
        send(region(o, psf, pse, psc), region(o, prf, pre, prc), bs.at[26 + n], br.at[26 + n], brick(*o))
        for n, o in enumerate(GHOSTS)
    ]

    for c in az_copies:
        c.wait_recv()
    arr[co, x, :, y] = g1[...]
    ax_copies = [
        send(g1, arr.at[co, x, :, y], axs.at[n], axr.at[n], xy_dev(s)) for n, s in enumerate(xy_steps)
    ]

    dr = drad_s[...]
    dr = dr[0:NB, 0:CH] + (dr[NB : 2 * NB, 0:CH] + dr[0:NB, CH : 2 * CH]) + dr[NB : 2 * NB, CH : 2 * CH]

    def blocks_of(o):
        view = [range(3) if c == 0 else [1 - c] for c in o]
        return [9 * i + 3 * k + l for i in view[0] for k in view[1] for l in view[2]]

    for n, o in enumerate(GHOSTS):
        back_copies[n].wait_recv()
    for o in GHOSTS:
        got = region(o, rf, re, rc)[...].astype(f32).reshape(-1, 8, 128)
        for n, b in enumerate(blocks_of(o)):
            own_s[b] += got[n]
    own = own_s[...]
    own = jnp.concatenate([own[:, None, :, 0:CH], own[:, None, :, CH : 2 * CH]], axis=1)
    own = jnp.transpose(own.reshape(ATOMS, CH))
    zscaled = (own * gains_s[...]).astype(bf16)
    weight = dot_nt(h_ref[...], zscaled)
    small = jnp.concatenate(
        [
            jnp.concatenate([weight[0:32], weight[32:64]], axis=1),
            jnp.concatenate([dr[0:8], dr[8:16]], axis=1),
            jnp.zeros((8, 128), f32),
        ],
        axis=0,
    )
    ar_l[...] = small.reshape(2, 24, 128)
    rc_copy = send(ar_l.at[nc - 1 - co], ar_r, rcs.at[0], rcr.at[0], sibling)

    for n, o in enumerate(GHOSTS):
        back_copies[26 + n].wait_recv()
    for o in GHOSTS:
        got = region(o, prf, pre, prc)[...].reshape(-1, 1, 128)
        for n, b in enumerate(blocks_of(o)):
            ownp_s[b] += got[n]
    rc_copy.wait_recv()
    ar_x[x * ny + y] = (ar_l[co] + ar_r[...]).astype(bf16)
    rx_copies = [
        send(ar_x.at[x * ny + y], ar_x.at[x * ny + y], rxs.at[n], rxr.at[n], xy_dev(s))
        for n, s in enumerate(xy_steps)
    ]
    ownp = jnp.transpose(ownp_s[...].reshape(32, 128))[0:48]
    wide = dot_nn(jnp.concatenate(split3(ownp), axis=1), jnp.concatenate([block_hot] * 3, axis=0))
    ownp = jnp.concatenate(
        [
            jnp.sum(jnp.where(in_block, wide[16 * d : 16 * d + 16], 0.0), axis=0, keepdims=True)
            for d in range(3)
        ],
        axis=0,
    )
    pos_s[...] = ownp - ownpos_s[0:3]
    ew_s[...] = dy_ref[...].astype(f32) + dot_nn(mix_ref[...], zscaled)

    for c in ax_copies:
        c.wait_recv()
    ac_copy = send(arr.at[co], arr.at[co], acs.at[0], acr.at[0], sibling)

    ep_s[...] = jnp.zeros((16, ATOMS), f32)

    per_x = per_core // nx

    def ewald_one(step):
        n = lax.rem(step + co * per_core, 2 * per_core)
        rows_n = chunk * 2 * ROWS
        m = lax.rem(n, per_core)
        run = nl // per_x
        co_n = arr[n // per_core, m // per_x, pl.ds(lax.rem(m, per_x) * run, run)].reshape(rows_n, 128)
        cs_n = cs[pl.ds(pl.multiple_of(n * rows_n, rows_n), rows_n), :]
        along = dot_nn(co_n, st_s[...]).reshape(chunk, 2, ROWS, ATOMS)
        trig = cs_n.astype(f32).reshape(chunk, 2, ROWS, ATOMS)
        ag = (along[:, 1] * trig[:, 0] - along[:, 0] * trig[:, 1]).reshape(chunk * ROWS, ATOMS)
        m_n = mi_s[:, pl.ds(pl.multiple_of(n * (chunk * ROWS), chunk * ROWS), chunk * ROWS)]
        co_t = jnp.transpose(co_n.astype(f32))[0:CH].astype(bf16)
        return (
            dot_nn(co_t, cs_n),
            dot_nn(jnp.concatenate([m_n, m_n], axis=1), jnp.concatenate(split2(ag), axis=0)),
        )

    def ewald_step(step, _):
        parts = [ewald_one(step * EWALD + k) for k in range(EWALD)]
        ew_s[...] += functools.reduce(jnp.add, [p[0] for p in parts])
        ep_s[...] += functools.reduce(jnp.add, [p[1] for p in parts])
        return 0

    steps = devices // chunk // EWALD
    lax.fori_loop(0, steps // 2, ewald_step, 0)
    for c in rx_copies:
        c.wait_recv()
    part = ar_x[0].astype(f32)
    for n in range(1, nx * ny):
        part = part + ar_x[n].astype(f32)
    ar_z[zl * nh + zh] = part
    rz_copies = [
        send(ar_z.at[zl * nh + zh], ar_z.at[zl * nh + zh], rzs.at[n], rzr.at[n], z_dev(s))
        for n, s in enumerate(z_steps)
    ]
    ac_copy.wait_recv()
    lax.fori_loop(steps // 2, steps, ewald_step, 0)
    atom_out[...] = ew_s[...].astype(bf16)
    ep = ep_s[0:3]
    turn = 2.0 * math.pi
    pos_out[:, 0, :] = pos_s[...] + jnp.concatenate(
        [ep[0:1] * (turn / nx), ep[1:2] * (turn / n_gy), ep[2:3] * (turn / n_gz)], axis=0
    )

    for c in rz_copies:
        c.wait_recv()
    part = ar_z[0]
    for n in range(1, nl * nh):
        part = part + ar_z[n]
    ar_o[co] = part
    ro_copy = send(ar_o.at[co], ar_o.at[co], ros.at[0], ror.at[0], sibling)
    ro_copy.wait_recv()
    full = ar_o[...].reshape(48, 128)
    weight_out[...] = jnp.concatenate([full[0:32, 0:CH], full[0:32, CH : 2 * CH]], axis=0)
    radial_out[...] = jnp.concatenate([full[32:40, 0:CH], full[32:40, CH : 2 * CH]], axis=0)

    for c in (
        ghost_copies + [core_copy] + xy_copies + z_copies + az_copies + ax_copies + back_copies
        + [rc_copy, ac_copy] + rx_copies + rz_copies + [ro_copy]
    ):
        c.wait_send()


def deliver_kernel(*refs):
    n = (len(refs) - 1) // 3
    copies = [pltpu.make_async_copy(refs[i], refs[2 * n + i], refs[-1].at[i]) for i in range(n)]
    for c in copies:
        c.start()
    for c in copies:
        c.wait()
    for i in range(n):
        refs[n + i][...] = refs[2 * n + i][...]


def deliver(arrays):
    return pl.pallas_call(
        deliver_kernel,
        out_shape=tuple(jax.ShapeDtypeStruct(a.shape, a.dtype) for a in arrays),
        in_specs=[pl.BlockSpec(memory_space=pl.ANY)] * len(arrays),
        out_specs=(pl.BlockSpec(memory_space=pltpu.VMEM),) * len(arrays),
        scratch_shapes=[pltpu.VMEM(a.shape, a.dtype) for a in arrays]
        + [pltpu.SemaphoreType.DMA((len(arrays),))],
        compiler_params=pltpu.CompilerParams(vmem_limit_bytes=62 * 1024 * 1024),
        name="deliver",
    )(*arrays)


def shards(sizes, h, dy, pos, labels, entries, miller, kfilter, mix, table, radial):
    nx, nl, ny, nh, nc = sizes
    devices = nx * nl * ny * nh * nc
    k = ROWS * devices
    nxy, nz = nx * ny, nl * nh
    vmem = pl.BlockSpec(memory_space=pltpu.VMEM)
    dma = pltpu.SemaphoreType.DMA
    plane = devices // nc
    scratch = [
        pltpu.VMEM((2 * k, ATOMS), bf16),
        pltpu.VMEM((nc, plane, 16, 128), f32),
        pltpu.VMEM((nc, nx, nl, ny, nh, 16, 128), bf16),
        pltpu.VMEM((3, 3, 3, 8, 128), bf16),
        pltpu.VMEM((5, 8, 128), bf16),
        pltpu.VMEM((6, 3, 3, 8, 128), bf16),
        pltpu.VMEM((12, 3, 8, 128), bf16),
        pltpu.VMEM((8, 8, 128), bf16),
        pltpu.VMEM((3, 3, 3, 1, 128), f32),
        pltpu.VMEM((5, 1, 128), f32),
    ]
    for _ in range(3):
        scratch += [
            pltpu.VMEM((6, 3, 3, 1, 128), f32),
            pltpu.VMEM((12, 3, 1, 128), f32),
            pltpu.VMEM((8, 1, 128), f32),
        ]
    scratch += [
        pltpu.VMEM((4 * CH, SEG), bf16),
        pltpu.VMEM((BLOCKS, 128), f32),
        pltpu.VMEM((NBR // GROUP, BLOCKS, GROUP * ATOMS), bf16),
        pltpu.VMEM((96, GROUP * ATOMS), bf16),
        pltpu.VMEM((BLOCKS, 96), f32),
        pltpu.VMEM((32, 1, 128), f32),
        pltpu.VMEM((NBR, 8, ATOMS), i32),
        pltpu.VMEM((NBR // GROUP, SEG, GROUP * ATOMS), bf16),
        pltpu.VMEM((NBR, CH, ATOMS), bf16),
        pltpu.VMEM((NBR, CH, ATOMS), f32),
        pltpu.VMEM((NBR, NB, ATOMS), f32),
        pltpu.VMEM((NBR, 8, ATOMS), f32),
        pltpu.VMEM((4 * CH, GROUP * ATOMS), bf16),
        pltpu.VMEM((CH, ATOMS), f32),
        pltpu.VMEM((SEG, 4 * CH), f32),
        pltpu.VMEM((32, 8, 128), f32),
        pltpu.VMEM((8, ATOMS), f32),
        pltpu.VMEM((CH, ATOMS), f32),
        pltpu.VMEM((2 * NB, 2 * CH), f32),
        pltpu.VMEM((6, 3, 3, 8, 128), bf16),
        pltpu.VMEM((12, 3, 8, 128), bf16),
        pltpu.VMEM((8, 8, 128), bf16),
        pltpu.VMEM((6, 3, 3, 8, 128), bf16),
        pltpu.VMEM((12, 3, 8, 128), bf16),
        pltpu.VMEM((8, 8, 128), bf16),
        pltpu.VMEM((plane, 16, 128), f32),
        pltpu.VMEM((nx, nl, ny, nh, 16, 128), bf16),
        pltpu.VMEM((nxy - 1, nl, nh, 16, 128), bf16),
        pltpu.VMEM((nl, nh, 16, 128), f32),
        pltpu.VMEM((nz - 1, 16, 128), f32),
        pltpu.VMEM((nl, nh, 16, 128), bf16),
        pltpu.VMEM((k, 16), bf16),
        pltpu.VMEM((16, ATOMS), bf16),
        pltpu.VMEM((2 * CH, ATOMS), bf16),
        pltpu.VMEM((ATOMS, 2 * CH), bf16),
        pltpu.VMEM((CH, ATOMS), f32),
        pltpu.VMEM((CH, ATOMS), f32),
        pltpu.VMEM((16, ATOMS), f32),
        pltpu.VMEM((CH, 128), f32),
        pltpu.VMEM((128, CH), f32),
        pltpu.VMEM((16, k), bf16),
        pltpu.VMEM((8, 128), f32),
        pltpu.VMEM((3, ATOMS), f32),
        pltpu.VMEM((2, 24, 128), f32),
        pltpu.VMEM((24, 128), f32),
        pltpu.VMEM((nxy, 24, 128), bf16),
        pltpu.VMEM((nz, 24, 128), f32),
        pltpu.VMEM((2, 24, 128), f32),
        pltpu.VMEM((CH, ATOMS), bf16),
        pltpu.VMEM((CH, ATOMS), bf16),
        pltpu.VMEM((3, 1, ATOMS), f32),
        pltpu.VMEM((1, ATOMS), i32),
        pltpu.VMEM((NBR, ATOMS), i32),
        pltpu.VMEM((3, k), i32),
        pltpu.VMEM((CH, CH), bf16),
        pltpu.VMEM((4, CH), f32),
        pltpu.VMEM((NB, CH), f32),
        dma((9,)),
        dma,
    ]
    for count in (52, 52, 1, nxy - 1, nz - 1, nz - 1, nxy - 1, 1, 1, nxy - 1, nz - 1, 1):
        scratch += [dma((count,)), dma((count,))]
    out = pl.pallas_call(
        functools.partial(kernel, sizes),
        out_shape=(
            jax.ShapeDtypeStruct((CH, ATOMS), bf16),
            jax.ShapeDtypeStruct((3, 1, ATOMS), f32),
            jax.ShapeDtypeStruct((CH, CH), f32),
            jax.ShapeDtypeStruct((NB, CH), f32),
            jax.ShapeDtypeStruct((ROWS, CH), f32),
        ),
        in_specs=[pl.BlockSpec(memory_space=pl.ANY)] * 10,
        out_specs=(vmem,) * 5,
        scratch_shapes=scratch,
        compiler_params=pltpu.CompilerParams(
            collective_id=0, has_side_effects=True, vmem_limit_bytes=62 * 1024 * 1024
        ),
        name="layer",
    )(
        h[0, 0, 0], dy[0, 0, 0], jnp.transpose(pos, (0, 1, 3, 2, 4))[0, 0], labels[0, 0], entries[0, 0, 0],
        miller, kfilter.T, mix, table, radial,
    )
    out = deliver(out)
    return (out[0][None, None, None], jnp.transpose(out[1][None, None], (0, 1, 3, 2, 4)), out[2], out[3], out[4])


def solution(mesh):
    sizes = (mesh.shape["gx"], 4, mesh.shape["gy"] // 4, mesh.shape["gz"] // 2, 2)
    finer = Mesh(mesh.devices.reshape(sizes), AXES)
    brick = P("gx", GY, GZ, None, None)
    return jax.shard_map(
        functools.partial(shards, sizes),
        mesh=finer,
        in_specs=(brick, brick, brick, P("gx", GY, GZ, None), brick, P(), P(), P(), P(), P()),
        out_specs=(brick, brick, P(), P(), P(AXES, None)),
        check_vma=False,
    )
```

```python
import functools
import math

import jax
import jax.numpy as jnp
from jax import lax
from jax.experimental import pallas as pl
from jax.experimental.pallas import tpu as pltpu
from jax.sharding import Mesh
from jax.sharding import PartitionSpec as P

AXES = ("gx", "gy_0", "gy_1", "gz_0", "gz_1")
GY = ("gy_0", "gy_1")
GZ = ("gz_0", "gz_1")
MESH = pl.DeviceIdType.MESH
f32, bf16, i32 = jnp.float32, jnp.bfloat16, jnp.int32

CH = 64
ATOMS = 512
NBR = 16
NB = 16
ROWS = 8
SEG = 528
BLOCKS = 144
EWALD = 4
GROUP = 8
reach_sq = 0.75

COS = (
    0.9999999890590228,
    -19.739204499454026,
    64.93911745990036,
    -85.45013953095037,
    60.16763095136588,
    -25.96759924965491,
    6.528658162567069,
)
SIN = (
    6.283185302511503,
    -41.34170040531769,
    81.60513138580204,
    -76.7030153539128,
    42.02592698618416,
    -14.899846668691637,
    3.238137510515757,
)

SLOTS = [(ox, oy, oz) for ox in (-1, 0, 1) for oy in (-1, 0, 1) for oz in (-1, 0, 1)]
FACES = [o for o in SLOTS if sum(map(abs, o)) == 1]
EDGES = [o for o in SLOTS if sum(map(abs, o)) == 2]
CORNERS = [o for o in SLOTS if sum(map(abs, o)) == 3]
GHOSTS = sorted(FACES + EDGES + CORNERS, key=lambda o: -abs(o[2]))


def base_block(o):
    if o in FACES:
        return 32 + 9 * FACES.index(o)
    if o in EDGES:
        return 32 + 54 + 3 * EDGES.index(o)
    if o in CORNERS:
        return 32 + 54 + 36 + CORNERS.index(o)
    return 0


def poly(coef, x):
    acc = jnp.full_like(x, coef[-1])
    for c in coef[-2::-1]:
        acc = acc * x + c
    return acc


def split2(x):
    hi = x.astype(bf16)
    return hi, (x - hi.astype(f32)).astype(bf16)


def split3(x):
    hi = x.astype(bf16)
    rest = x - hi.astype(f32)
    mid = rest.astype(bf16)
    return hi, mid, (rest - mid.astype(f32)).astype(bf16)


def dot_nn(a, b):
    return jnp.dot(a, b, preferred_element_type=f32)


def dot_nt(a, b):
    return lax.dot_general(a, b, (((1,), (1,)), ((), ())), preferred_element_type=f32)


def pick(ref, o):
    return ref.at[tuple(slice(None) if c == 0 else 1 - c for c in o)]


def region(o, faces, edges, corners):
    if o in FACES:
        return faces.at[FACES.index(o)]
    if o in EDGES:
        return edges.at[EDGES.index(o)]
    return corners.at[CORNERS.index(o)]


def kernel(
    sizes,
    h_in, dy_in, pos_in, lab_in, idx_in, mil_in, kf_ref, mix_in, gain_in, rad_in,
    atom_out, pos_out, weight_out, radial_out, filter_out,
    cs, tot, arr,
    feat, feat5, gf, ge, gc,
    pfeat, pfeat5, pgf, pge, pgc, psf, pse, psc, prf, pre, prc, table_s, xp_s, hotb, dgp, gradp_s, ownp_s,
    meta, onehot, near, filt, basis_s, rel_s, dgs, agg_s, grad_s, own_s, ownpos_s, u_s, drad_s,
    sf, se, sc, rf, re, rc,
    rec_a, a_bf, rec_b, sum_b, rec_c, g1,
    m9_s, p9_s, st_s, stt_s, gains_s, ew_s, ep_s, kf_s, kft_s, mi_s, tab_s, pos_s,
    ar_l, ar_r, ar_x, ar_z, ar_o,
    h_ref, dy_ref, pos_ref, lab_ref, idx_ref, mil_ref, mix_ref, gain_ref, rad_ref, in_sem,
    kf_sem, gs, gr, bs, br, cs_s, cs_r, xs, xr, zs, zr, azs, azr, axs, axr, acs, acr,
    rcs, rcr, rxs, rxr, rzs, rzr, ros, ror,
):
    nx, nl, ny, nh, nc = sizes
    x, zl, y, zh, co = (lax.axis_index(a) for a in AXES)
    devices = nx * nl * ny * nh * nc
    gy, gz = zl * ny + y, zh * nc + co
    n_gy, n_gz = nl * ny, nh * nc
    owner = ((x * nl + zl) * ny + y) * nh * nc + zh * nc + co
    norm_atoms = (ATOMS * devices) ** (-0.5)
    norm_k = (ROWS * devices) ** (-0.5)

    def brick(ox, oy, oz):
        bx = lax.rem(x + (ox + nx), nx)
        by = lax.rem(gy + (oy + n_gy), n_gy)
        bz = lax.rem(gz + (oz + n_gz), n_gz)
        return (bx, by // ny, lax.rem(by, ny), bz // nc, lax.rem(bz, nc))

    xy_steps = [(i, j) for i in range(nx) for j in range(ny) if (i, j) != (0, 0)]
    z_steps = [(i, j) for i in range(nh) for j in range(nl) if (i, j) != (0, 0)]

    def xy_to(step):
        return lax.rem(x + step[0], nx), lax.rem(y + step[1], ny)

    def z_to(step):
        return lax.rem(zh + step[0], nh), lax.rem(zl + step[1], nl)

    sibling = (x, zl, y, zh, nc - 1 - co)

    def xy_dev(step):
        tx, ty = xy_to(step)
        return (tx, zl, ty, zh, co)

    def z_dev(step):
        th, tl = z_to(step)
        return (x, tl, y, th, co)

    def send(src, dst, ssem, rsem, dev):
        copy = pltpu.make_async_remote_copy(
            src_ref=src, dst_ref=dst, send_sem=ssem, recv_sem=rsem, device_id=dev, device_id_type=MESH
        )
        copy.start()
        return copy

    in_copies = [
        pltpu.make_async_copy(a, b, in_sem.at[n])
        for n, (a, b) in enumerate(
            (
                (h_in, h_ref), (pos_in, pos_ref), (lab_in, lab_ref), (mix_in, mix_ref), (gain_in, gain_ref),
                (mil_in, mil_ref), (dy_in, dy_ref), (idx_in, idx_ref), (rad_in, rad_ref),
            )
        )
    ]
    for c in in_copies:
        c.start()
    kf_copy = pltpu.make_async_copy(kf_ref.at[:, pl.ds(pl.multiple_of(owner // 16 * 128, 128), 128)], kf_s, kf_sem)
    kf_copy.start()

    barrier = pltpu.get_barrier_semaphore()
    partners = [brick(*o) for o in GHOSTS] + [xy_dev(s) for s in xy_steps] + [z_dev(s) for s in z_steps] + [sibling]
    for dev in partners:
        pl.semaphore_signal(barrier, inc=1, device_id=dev, device_id_type=MESH)

    for c in in_copies:
        c.wait()

    hb = h_ref[...]
    tab_s[...] = jnp.zeros((8, 128), f32)
    tab_s[0:4, 0:CH] = gain_ref[...]
    tab = jnp.transpose(tab_s[...])[0:CH]
    lab = lab_ref[...]
    gains = jnp.zeros((CH, ATOMS), f32)
    for s in range(4):
        gains = jnp.where(lab == s, tab[:, s : s + 1], gains)
    gains_s[...] = gains
    mix = mix_ref[...]
    mix_t = jnp.transpose(mix.astype(f32)).astype(bf16)
    z = jnp.transpose((dot_nn(mix_t, hb) * gains).astype(bf16).astype(f32)).reshape(32, 2, 8, CH)
    z = jnp.concatenate([z[:, 0], z[:, 1]], axis=2).astype(bf16)
    feat[...] = z[0:27].reshape(3, 3, 3, 8, 128)
    feat5[...] = z[27:32]
    p = pos_ref[:, 0, :]
    pos_s[...] = p
    lane = lax.broadcasted_iota(i32, (16, ATOMS), 1)
    in_block = (lane & 15) == lax.broadcasted_iota(i32, (16, ATOMS), 0)
    block_hot = jnp.where(
        lax.broadcasted_iota(i32, (32, ATOMS), 1) >> 4 == lax.broadcasted_iota(i32, (32, ATOMS), 0), 1.0, 0.0
    ).astype(bf16)
    spread = jnp.concatenate([jnp.where(in_block, p[d : d + 1], 0.0) for d in range(3)], axis=0)
    parts = dot_nt(jnp.concatenate(split3(spread), axis=0), block_hot)
    parts = (parts[0:48] + parts[48:96]) + parts[96:144]
    parts = jnp.transpose(jnp.concatenate([parts, jnp.zeros((80, 32), f32)], axis=0))
    pfeat[...] = parts[0:27].reshape(3, 3, 3, 1, 128)
    pfeat5[...] = parts[27:32].reshape(5, 1, 128)

    st = jnp.concatenate([hb, dy_ref[...]], axis=0)
    st_s[...] = st
    stt_s[...] = jnp.transpose(st.astype(f32)).astype(bf16)
    mil = mil_ref[...].astype(f32)
    mrows = jnp.concatenate([mil, mil, mil, jnp.zeros((7, mil.shape[1]), f32)], axis=0)
    mrows = jnp.transpose(mrows).reshape(devices // nc, nc, ROWS, 16)
    mrows = jnp.concatenate([mrows[:, c] for c in range(nc)], axis=0).reshape(devices * ROWS, 16)
    m9_s[...] = mrows.astype(bf16)
    mi_s[...] = jnp.transpose(mrows).astype(bf16)
    absolute = jnp.concatenate(
        [
            (p[0:1] + x.astype(f32)) * (1.0 / nx),
            (p[1:2] + gy.astype(f32)) * (1.0 / n_gy),
            (p[2:3] + gz.astype(f32)) * (1.0 / n_gz),
        ],
        axis=0,
    )
    w_hi = absolute.astype(bf16).astype(f32)
    w_mid = (absolute - w_hi).astype(bf16).astype(f32)
    w_lo = (absolute - w_hi - w_mid).astype(bf16).astype(f32)
    p9_s[...] = jnp.concatenate([w_hi, w_mid, w_lo, jnp.zeros((7, ATOMS), f32)], axis=0).astype(bf16)

    chunk = 16
    per_core = devices // nc // chunk

    def phase_step(n, _):
        at = pl.multiple_of(n * (chunk * ROWS), chunk * ROWS)
        t = dot_nn(m9_s[pl.ds(at, chunk * ROWS), :], p9_s[...])
        t = t - jnp.floor(t + 0.5)
        sq = t * t
        cosine = poly(COS, sq).reshape(chunk, ROWS, ATOMS)
        sine = (t * poly(SIN, sq)).reshape(chunk, ROWS, ATOMS)
        both = jnp.concatenate([cosine, sine], axis=1).reshape(chunk * 2 * ROWS, ATOMS).astype(bf16)
        cs[pl.ds(pl.multiple_of(n * (chunk * 2 * ROWS), chunk * 2 * ROWS), chunk * 2 * ROWS), :] = both
        part = dot_nn(both, stt_s[...])
        tot[n // per_core, pl.ds(lax.rem(n, per_core) * chunk, chunk)] = part.reshape(chunk, 16, 128)
        return 0

    lax.fori_loop(0, devices // chunk, phase_step, 0)

    pl.semaphore_wait(barrier, len(partners))
    core_copy = send(tot.at[nc - 1 - co], rec_a, cs_s.at[0], cs_r.at[0], sibling)

    ghost_copies = [
        send(pick(feat, o), region(o, gf, ge, gc), gs.at[n], gr.at[n], brick(-o[0], -o[1], -o[2]))
        for n, o in enumerate(GHOSTS)
    ] + [
        send(pick(pfeat, o), region(o, pgf, pge, pgc), gs.at[26 + n], gr.at[26 + n], brick(-o[0], -o[1], -o[2]))
        for n, o in enumerate(GHOSTS)
    ]

    e = idx_ref[...]
    slot, atom = e >> 9, e & 511
    block = atom >> 4
    o1 = (slot * 57) >> 9
    o2 = ((slot - 9 * o1) * 11) >> 5
    o3 = slot - 9 * o1 - 3 * o2
    c1 = (block * 57) >> 9
    c2 = ((block - 9 * c1) * 11) >> 5
    c3 = block - 9 * c1 - 3 * c2
    place = jnp.zeros_like(e)
    for o_n, c_n in ((o1, c1), (o2, c2), (o3, c3)):
        place = jnp.where(o_n == 1, place * 3 + c_n, place)
    base = jnp.zeros_like(e)
    for n, o in enumerate(SLOTS):
        base = jnp.where(slot == n, base_block(o), base)
    at_block = jnp.where(slot == 13, block, base + place)
    inner = atom & 15
    row = at_block * 8 + (inner & 7)
    upper = jnp.where(row >= 512, 1, 0)
    low = row - 512 * upper
    segment = 2 * upper + (inner >> 3)
    for j in range(NBR):
        meta[j] = jnp.concatenate(
            [v[j : j + 1] for v in (low, segment, at_block, inner, o1 - 1, o2 - 1, o3 - 1)]
            + [jnp.zeros((1, ATOMS), i32)],
            axis=0,
        )

    core_copy.wait_recv()

    def core_sum(n, _):
        part = tot[co, pl.ds(n * (nl * ny * nh), nl * ny * nh)] + rec_a[pl.ds(n * (nl * ny * nh), nl * ny * nh)]
        a_bf[n] = part.astype(bf16).reshape(nl, ny, nh, 16, 128)
        return 0

    lax.fori_loop(0, nx, core_sum, 0)

    xy_copies = []
    for n, s in enumerate(xy_steps):
        tx, ty = xy_to(s)
        xy_copies.append(send(a_bf.at[tx, :, ty], rec_b.at[n], xs.at[n], xr.at[n], xy_dev(s)))

    def hot_step(n, _):
        for k in range(GROUP):
            m = meta[n * GROUP + k]
            at = slice(k * ATOMS, (k + 1) * ATOMS)
            onehot[n, :, at] = jnp.where(
                lax.broadcasted_iota(i32, (SEG, ATOMS), 0) == m[0:1], 1.0, 0.0
            ).astype(bf16)
            hotb[n, :, at] = jnp.where(
                lax.broadcasted_iota(i32, (BLOCKS, ATOMS), 0) == m[2:3], 1.0, 0.0
            ).astype(bf16)
        return 0

    lax.fori_loop(0, NBR // GROUP, hot_step, 0)

    for c in ghost_copies:
        c.wait_recv()

    table = jnp.concatenate(
        [
            feat[...].reshape(216, 128),
            feat5[...].reshape(40, 128),
            gf[...].reshape(432, 128),
            ge[...].reshape(288, 128),
            gc[...].reshape(64, 128),
        ],
        axis=0,
    ).astype(f32)
    table = jnp.concatenate(
        [
            jnp.concatenate([jnp.transpose(table[0:512]), jnp.zeros((128, SEG - 512), f32)], axis=1),
            jnp.transpose(table[512:1040]),
        ],
        axis=0,
    )
    table_s[...] = table.astype(bf16)
    xp_s[...] = jnp.zeros((BLOCKS, 128), f32)
    xp_s[0:27] = pfeat[...].reshape(27, 128)
    xp_s[27:32] = pfeat5[...].reshape(5, 128)
    xp_s[32:86] = pgf[...].reshape(54, 128)
    xp_s[86:122] = pge[...].reshape(36, 128)
    xp_s[122:130] = pgc[...].reshape(8, 128)
    ptable = jnp.concatenate(split3(jnp.transpose(xp_s[...])[0:48]), axis=0)
    rad = rad_ref[...]
    rad_hi, rad_lo = split2(rad)
    radt_hi, radt_lo = split2(jnp.transpose(rad))
    rad_fwd = jnp.concatenate([radt_hi, radt_hi, radt_lo], axis=1)
    rad_bwd = jnp.concatenate([rad_hi, rad_hi, rad_lo], axis=1)
    spacing = reach_sq / (NB - 1)
    centres = lax.broadcasted_iota(i32, (NB, ATOMS), 0).astype(f32) * spacing
    agg_s[...] = jnp.zeros((CH, ATOMS), f32)

    def forward_one(n, k):
        j = n * GROUP + k
        m = meta[j]
        seg_j = m[1:2]
        at = slice(k * ATOMS, (k + 1) * ATOMS)
        got = dot_nn(table_s[...], onehot[n, :, at])
        nz = jnp.where(
            seg_j < 2,
            jnp.where(seg_j == 0, got[0:CH], got[CH : 2 * CH]),
            jnp.where(seg_j == 2, got[2 * CH : 3 * CH], got[3 * CH : 4 * CH]),
        )
        near[j] = nz.astype(bf16)
        gotp = dot_nn(ptable, hotb[n, :, at])
        gotp = (gotp[0:48] + gotp[48:96]) + gotp[96:144]
        mine = lax.broadcasted_iota(i32, (16, ATOMS), 0) == m[3:4]
        near_pos = jnp.concatenate(
            [
                jnp.sum(jnp.where(mine, gotp[16 * d : 16 * d + 16], 0.0), axis=0, keepdims=True)
                for d in range(3)
            ],
            axis=0,
        )
        rel = (near_pos + m[4:7].astype(f32)) - pos_s[...]
        sq = rel * rel
        dist = sq[0:1] + sq[1:2] + sq[2:3]
        rel_s[j] = jnp.concatenate([rel, dist, jnp.zeros((4, ATOMS), f32)], axis=0)
        d = (dist - centres) / (2.0 * spacing)
        b = jnp.exp(-(d * d))
        basis_s[j] = b
        b_hi, b_lo = split2(b)
        fl = dot_nn(rad_fwd, jnp.concatenate([b_hi, b_lo, b_hi], axis=0))
        filt[j] = fl
        return fl * nz

    def forward_step(n, _):
        parts = [forward_one(n, k) for k in range(GROUP)]
        agg_s[...] += functools.reduce(jnp.add, parts)
        return 0

    half = NBR // GROUP // 2
    lax.fori_loop(0, half, forward_step, 0)

    for c in xy_copies:
        c.wait_recv()
    part = a_bf[x, :, y].astype(f32)
    for n in range(len(xy_steps)):
        part = part + rec_b[n].astype(f32)
    sum_b[...] = part

    z_copies = []
    for n, s in enumerate(z_steps):
        th, tl = z_to(s)
        z_copies.append(send(sum_b.at[tl, th], rec_c.at[n], zs.at[n], zr.at[n], z_dev(s)))

    lax.fori_loop(half, NBR // GROUP, forward_step, 0)

    v = agg_s[...] * NBR ** (-0.5)
    sig = 1.0 / (1.0 + jnp.exp(-v))
    u_s[...] = dy_ref[...].astype(f32) * (sig * (1.0 + v * (1.0 - sig))) * NBR ** (-0.5)

    grad_s[...] = jnp.zeros((SEG, 4 * CH), f32)
    gradp_s[...] = jnp.zeros((BLOCKS, 96), f32)
    ownpos_s[...] = jnp.zeros((8, ATOMS), f32)
    drad_s[...] = jnp.zeros((2 * NB, 2 * CH), f32)

    def backward_one(j, k):
        u = u_s[...]
        nz = near[j].astype(f32)
        dz = u * filt[j]
        df = u * nz
        df_hi, df_lo = split2(df)
        b = basis_s[j]
        b_hi, b_lo = split2(b)
        db = dot_nn(rad_bwd, jnp.concatenate([df_hi, df_lo, df_hi], axis=0))
        drad = dot_nt(jnp.concatenate([b_hi, b_lo], axis=0), jnp.concatenate([df_hi, df_lo], axis=0))
        r = rel_s[j]
        d = (r[3:4] - centres) / (2.0 * spacing)
        ddist = jnp.sum(db * b * d, axis=0, keepdims=True) * (-2.0 / (2.0 * spacing))
        drel = 2.0 * r[0:3] * ddist
        m = meta[j]
        seg_j = m[1:2]
        at = slice(k * ATOMS, (k + 1) * ATOMS)
        dgs[:, at] = jnp.concatenate([jnp.where(seg_j == q, dz, 0.0) for q in range(4)], axis=0).astype(bf16)
        drel_hi = drel.astype(bf16).astype(f32)
        mine = lax.broadcasted_iota(i32, (16, ATOMS), 0) == m[3:4]
        dgp[:, at] = jnp.concatenate(
            [jnp.where(mine, v[d : d + 1], 0.0) for v in (drel_hi, drel - drel_hi) for d in range(3)], axis=0
        ).astype(bf16)
        return drad, drel

    def backward_step(n, _):
        parts = [backward_one(n * GROUP + k, k) for k in range(GROUP)]
        drad_s[...] += functools.reduce(jnp.add, [p[0] for p in parts])
        ownpos_s[0:3] += functools.reduce(jnp.add, [p[1] for p in parts])
        grad_s[...] += dot_nt(onehot[n], dgs[...])
        gradp_s[...] += dot_nt(hotb[n], dgp[...])
        return 0

    lax.fori_loop(0, half, backward_step, 0)

    for c in z_copies:
        c.wait_recv()
    total = sum_b[zl, zh]
    for n in range(len(z_steps)):
        total = total + rec_c[n]
    kf_copy.wait()
    kft_s[...] = jnp.transpose(kf_s[...])
    kf = kft_s[pl.ds(pl.multiple_of(lax.rem(owner, 16) * ROWS, ROWS), ROWS), :]
    struct = total[:, 0:CH] * norm_atoms
    back = total[:, CH : 2 * CH] * norm_k
    prod = struct * back
    filter_out[...] = prod[0:ROWS] + prod[ROWS : 2 * ROWS]
    kf2 = jnp.concatenate([kf, kf], axis=0)
    coeffs = jnp.concatenate([norm_atoms * kf2 * back, norm_k * kf2 * struct], axis=1).astype(bf16)
    g1[zl, zh] = coeffs
    az_copies = [
        send(g1.at[zl, zh], g1.at[zl, zh], azs.at[n], azr.at[n], z_dev(s)) for n, s in enumerate(z_steps)
    ]

    lax.fori_loop(half, NBR // GROUP, backward_step, 0)

    grad = grad_s[...]
    grad = jnp.concatenate([grad[0:512, 0:128], grad[:, 128:256]], axis=0)
    own_s[...] = grad[0:256].reshape(32, 8, 128)
    sf[...] = grad[256:688].astype(bf16).reshape(6, 3, 3, 8, 128)
    se[...] = grad[688:976].astype(bf16).reshape(12, 3, 8, 128)
    sc[...] = grad[976:1040].astype(bf16).reshape(8, 8, 128)
    gradp = gradp_s[...]
    gradp = jnp.concatenate([gradp[:, 0:48] + gradp[:, 48:96], jnp.zeros((BLOCKS, 80), f32)], axis=1)
    ownp_s[...] = gradp[0:32].reshape(32, 1, 128)
    psf[...] = gradp[32:86].reshape(6, 3, 3, 1, 128)
    pse[...] = gradp[86:122].reshape(12, 3, 1, 128)
    psc[...] = gradp[122:130].reshape(8, 1, 128)
    back_copies = [
        send(region(o, sf, se, sc), region(o, rf, re, rc), bs.at[n], br.at[n], brick(*o))
        for n, o in enumerate(GHOSTS)
    ] + [
        send(region(o, psf, pse, psc), region(o, prf, pre, prc), bs.at[26 + n], br.at[26 + n], brick(*o))
        for n, o in enumerate(GHOSTS)
    ]

    for c in az_copies:
        c.wait_recv()
    arr[co, x, :, y] = g1[...]
    ax_copies = [
        send(g1, arr.at[co, x, :, y], axs.at[n], axr.at[n], xy_dev(s)) for n, s in enumerate(xy_steps)
    ]

    dr = drad_s[...]
    dr = dr[0:NB, 0:CH] + (dr[NB : 2 * NB, 0:CH] + dr[0:NB, CH : 2 * CH]) + dr[NB : 2 * NB, CH : 2 * CH]

    def blocks_of(o):
        view = [range(3) if c == 0 else [1 - c] for c in o]
        return [9 * i + 3 * k + l for i in view[0] for k in view[1] for l in view[2]]

    for n, o in enumerate(GHOSTS):
        back_copies[n].wait_recv()
    for o in GHOSTS:
        got = region(o, rf, re, rc)[...].astype(f32).reshape(-1, 8, 128)
        for n, b in enumerate(blocks_of(o)):
            own_s[b] += got[n]
    own = own_s[...]
    own = jnp.concatenate([own[:, None, :, 0:CH], own[:, None, :, CH : 2 * CH]], axis=1)
    own = jnp.transpose(own.reshape(ATOMS, CH))
    zscaled = (own * gains_s[...]).astype(bf16)
    weight = dot_nt(h_ref[...], zscaled)
    small = jnp.concatenate(
        [
            jnp.concatenate([weight[0:32], weight[32:64]], axis=1),
            jnp.concatenate([dr[0:8], dr[8:16]], axis=1),
            jnp.zeros((8, 128), f32),
        ],
        axis=0,
    )
    ar_l[...] = small.reshape(2, 24, 128)
    rc_copy = send(ar_l.at[nc - 1 - co], ar_r, rcs.at[0], rcr.at[0], sibling)

    for n, o in enumerate(GHOSTS):
        back_copies[26 + n].wait_recv()
    for o in GHOSTS:
        got = region(o, prf, pre, prc)[...].reshape(-1, 1, 128)
        for n, b in enumerate(blocks_of(o)):
            ownp_s[b] += got[n]
    rc_copy.wait_recv()
    ar_x[x * ny + y] = (ar_l[co] + ar_r[...]).astype(bf16)
    rx_copies = [
        send(ar_x.at[x * ny + y], ar_x.at[x * ny + y], rxs.at[n], rxr.at[n], xy_dev(s))
        for n, s in enumerate(xy_steps)
    ]
    ownp = jnp.transpose(ownp_s[...].reshape(32, 128))[0:48]
    wide = dot_nn(jnp.concatenate(split3(ownp), axis=1), jnp.concatenate([block_hot] * 3, axis=0))
    ownp = jnp.concatenate(
        [
            jnp.sum(jnp.where(in_block, wide[16 * d : 16 * d + 16], 0.0), axis=0, keepdims=True)
            for d in range(3)
        ],
        axis=0,
    )
    pos_s[...] = ownp - ownpos_s[0:3]
    ew_s[...] = dy_ref[...].astype(f32) + dot_nn(mix_ref[...], zscaled)

    for c in ax_copies:
        c.wait_recv()
    ac_copy = send(arr.at[co], arr.at[co], acs.at[0], acr.at[0], sibling)

    ep_s[...] = jnp.zeros((16, ATOMS), f32)

    per_x = per_core // nx

    def ewald_one(step):
        n = lax.rem(step + co * per_core, 2 * per_core)
        rows_n = chunk * 2 * ROWS
        m = lax.rem(n, per_core)
        run = nl // per_x
        co_n = arr[n // per_core, m // per_x, pl.ds(lax.rem(m, per_x) * run, run)].reshape(rows_n, 128)
        cs_n = cs[pl.ds(pl.multiple_of(n * rows_n, rows_n), rows_n), :]
        along = dot_nn(co_n, st_s[...]).reshape(chunk, 2, ROWS, ATOMS)
        trig = cs_n.astype(f32).reshape(chunk, 2, ROWS, ATOMS)
        ag = (along[:, 1] * trig[:, 0] - along[:, 0] * trig[:, 1]).reshape(chunk * ROWS, ATOMS)
        m_n = mi_s[:, pl.ds(pl.multiple_of(n * (chunk * ROWS), chunk * ROWS), chunk * ROWS)]
        co_t = jnp.transpose(co_n.astype(f32))[0:CH].astype(bf16)
        return (
            dot_nn(co_t, cs_n),
            dot_nn(jnp.concatenate([m_n, m_n], axis=1), jnp.concatenate(split2(ag), axis=0)),
        )

    def ewald_step(step, _):
        parts = [ewald_one(step * EWALD + k) for k in range(EWALD)]
        ew_s[...] += functools.reduce(jnp.add, [p[0] for p in parts])
        ep_s[...] += functools.reduce(jnp.add, [p[1] for p in parts])
        return 0

    steps = devices // chunk // EWALD
    lax.fori_loop(0, steps // 2, ewald_step, 0)
    for c in rx_copies:
        c.wait_recv()
    part = ar_x[0].astype(f32)
    for n in range(1, nx * ny):
        part = part + ar_x[n].astype(f32)
    ar_z[zl * nh + zh] = part
    rz_copies = [
        send(ar_z.at[zl * nh + zh], ar_z.at[zl * nh + zh], rzs.at[n], rzr.at[n], z_dev(s))
        for n, s in enumerate(z_steps)
    ]
    ac_copy.wait_recv()
    lax.fori_loop(steps // 2, steps, ewald_step, 0)
    atom_out[...] = ew_s[...].astype(bf16)
    ep = ep_s[0:3]
    turn = 2.0 * math.pi
    pos_out[:, 0, :] = pos_s[...] + jnp.concatenate(
        [ep[0:1] * (turn / nx), ep[1:2] * (turn / n_gy), ep[2:3] * (turn / n_gz)], axis=0
    )

    for c in rz_copies:
        c.wait_recv()
    part = ar_z[0]
    for n in range(1, nl * nh):
        part = part + ar_z[n]
    ar_o[co] = part
    ro_copy = send(ar_o.at[co], ar_o.at[co], ros.at[0], ror.at[0], sibling)
    ro_copy.wait_recv()
    full = ar_o[...].reshape(48, 128)
    weight_out[...] = jnp.concatenate([full[0:32, 0:CH], full[0:32, CH : 2 * CH]], axis=0)
    radial_out[...] = jnp.concatenate([full[32:40, 0:CH], full[32:40, CH : 2 * CH]], axis=0)

    for c in (
        ghost_copies + [core_copy] + xy_copies + z_copies + az_copies + ax_copies + back_copies
        + [rc_copy, ac_copy] + rx_copies + rz_copies + [ro_copy]
    ):
        c.wait_send()


def deliver_kernel(*refs):
    n = (len(refs) - 1) // 2
    copies = [pltpu.make_async_copy(refs[i], refs[n + i], refs[-1].at[i]) for i in range(n)]
    for c in copies:
        c.start()
    for c in copies:
        c.wait()


def deliver(arrays):
    return pl.pallas_call(
        deliver_kernel,
        out_shape=tuple(jax.ShapeDtypeStruct(a.shape, a.dtype) for a in arrays),
        in_specs=[pl.BlockSpec(memory_space=pl.ANY)] * len(arrays),
        out_specs=(pl.BlockSpec(memory_space=pltpu.VMEM),) * len(arrays),
        scratch_shapes=[pltpu.SemaphoreType.DMA((len(arrays),))],
        compiler_params=pltpu.CompilerParams(vmem_limit_bytes=62 * 1024 * 1024),
        name="deliver",
    )(*arrays)


def shards(sizes, h, dy, pos, labels, entries, miller, kfilter, mix, table, radial):
    nx, nl, ny, nh, nc = sizes
    devices = nx * nl * ny * nh * nc
    k = ROWS * devices
    nxy, nz = nx * ny, nl * nh
    vmem = pl.BlockSpec(memory_space=pltpu.VMEM)
    dma = pltpu.SemaphoreType.DMA
    plane = devices // nc
    scratch = [
        pltpu.VMEM((2 * k, ATOMS), bf16),
        pltpu.VMEM((nc, plane, 16, 128), f32),
        pltpu.VMEM((nc, nx, nl, ny, nh, 16, 128), bf16),
        pltpu.VMEM((3, 3, 3, 8, 128), bf16),
        pltpu.VMEM((5, 8, 128), bf16),
        pltpu.VMEM((6, 3, 3, 8, 128), bf16),
        pltpu.VMEM((12, 3, 8, 128), bf16),
        pltpu.VMEM((8, 8, 128), bf16),
        pltpu.VMEM((3, 3, 3, 1, 128), f32),
        pltpu.VMEM((5, 1, 128), f32),
    ]
    for _ in range(3):
        scratch += [
            pltpu.VMEM((6, 3, 3, 1, 128), f32),
            pltpu.VMEM((12, 3, 1, 128), f32),
            pltpu.VMEM((8, 1, 128), f32),
        ]
    scratch += [
        pltpu.VMEM((4 * CH, SEG), bf16),
        pltpu.VMEM((BLOCKS, 128), f32),
        pltpu.VMEM((NBR // GROUP, BLOCKS, GROUP * ATOMS), bf16),
        pltpu.VMEM((96, GROUP * ATOMS), bf16),
        pltpu.VMEM((BLOCKS, 96), f32),
        pltpu.VMEM((32, 1, 128), f32),
        pltpu.VMEM((NBR, 8, ATOMS), i32),
        pltpu.VMEM((NBR // GROUP, SEG, GROUP * ATOMS), bf16),
        pltpu.VMEM((NBR, CH, ATOMS), bf16),
        pltpu.VMEM((NBR, CH, ATOMS), f32),
        pltpu.VMEM((NBR, NB, ATOMS), f32),
        pltpu.VMEM((NBR, 8, ATOMS), f32),
        pltpu.VMEM((4 * CH, GROUP * ATOMS), bf16),
        pltpu.VMEM((CH, ATOMS), f32),
        pltpu.VMEM((SEG, 4 * CH), f32),
        pltpu.VMEM((32, 8, 128), f32),
        pltpu.VMEM((8, ATOMS), f32),
        pltpu.VMEM((CH, ATOMS), f32),
        pltpu.VMEM((2 * NB, 2 * CH), f32),
        pltpu.VMEM((6, 3, 3, 8, 128), bf16),
        pltpu.VMEM((12, 3, 8, 128), bf16),
        pltpu.VMEM((8, 8, 128), bf16),
        pltpu.VMEM((6, 3, 3, 8, 128), bf16),
        pltpu.VMEM((12, 3, 8, 128), bf16),
        pltpu.VMEM((8, 8, 128), bf16),
        pltpu.VMEM((plane, 16, 128), f32),
        pltpu.VMEM((nx, nl, ny, nh, 16, 128), bf16),
        pltpu.VMEM((nxy - 1, nl, nh, 16, 128), bf16),
        pltpu.VMEM((nl, nh, 16, 128), f32),
        pltpu.VMEM((nz - 1, 16, 128), f32),
        pltpu.VMEM((nl, nh, 16, 128), bf16),
        pltpu.VMEM((k, 16), bf16),
        pltpu.VMEM((16, ATOMS), bf16),
        pltpu.VMEM((2 * CH, ATOMS), bf16),
        pltpu.VMEM((ATOMS, 2 * CH), bf16),
        pltpu.VMEM((CH, ATOMS), f32),
        pltpu.VMEM((CH, ATOMS), f32),
        pltpu.VMEM((16, ATOMS), f32),
        pltpu.VMEM((CH, 128), f32),
        pltpu.VMEM((128, CH), f32),
        pltpu.VMEM((16, k), bf16),
        pltpu.VMEM((8, 128), f32),
        pltpu.VMEM((3, ATOMS), f32),
        pltpu.VMEM((2, 24, 128), f32),
        pltpu.VMEM((24, 128), f32),
        pltpu.VMEM((nxy, 24, 128), bf16),
        pltpu.VMEM((nz, 24, 128), f32),
        pltpu.VMEM((2, 24, 128), f32),
        pltpu.VMEM((CH, ATOMS), bf16),
        pltpu.VMEM((CH, ATOMS), bf16),
        pltpu.VMEM((3, 1, ATOMS), f32),
        pltpu.VMEM((1, ATOMS), i32),
        pltpu.VMEM((NBR, ATOMS), i32),
        pltpu.VMEM((3, k), i32),
        pltpu.VMEM((CH, CH), bf16),
        pltpu.VMEM((4, CH), f32),
        pltpu.VMEM((NB, CH), f32),
        dma((9,)),
        dma,
    ]
    for count in (52, 52, 1, nxy - 1, nz - 1, nz - 1, nxy - 1, 1, 1, nxy - 1, nz - 1, 1):
        scratch += [dma((count,)), dma((count,))]
    out = pl.pallas_call(
        functools.partial(kernel, sizes),
        out_shape=(
            jax.ShapeDtypeStruct((CH, ATOMS), bf16),
            jax.ShapeDtypeStruct((3, 1, ATOMS), f32),
            jax.ShapeDtypeStruct((CH, CH), f32),
            jax.ShapeDtypeStruct((NB, CH), f32),
            jax.ShapeDtypeStruct((ROWS, CH), f32),
        ),
        in_specs=[pl.BlockSpec(memory_space=pl.ANY)] * 10,
        out_specs=(vmem,) * 5,
        scratch_shapes=scratch,
        compiler_params=pltpu.CompilerParams(
            collective_id=0, has_side_effects=True, vmem_limit_bytes=62 * 1024 * 1024
        ),
        name="layer",
    )(
        h[0, 0, 0], dy[0, 0, 0], jnp.transpose(pos, (0, 1, 3, 2, 4))[0, 0], labels[0, 0], entries[0, 0, 0],
        miller, kfilter.T, mix, table, radial,
    )
    out = deliver(out)
    return (out[0][None, None, None], jnp.transpose(out[1][None, None], (0, 1, 3, 2, 4)), out[2], out[3], out[4])


def solution(mesh):
    sizes = (mesh.shape["gx"], 4, mesh.shape["gy"] // 4, mesh.shape["gz"] // 2, 2)
    finer = Mesh(mesh.devices.reshape(sizes), AXES)
    brick = P("gx", GY, GZ, None, None)
    return jax.shard_map(
        functools.partial(shards, sizes),
        mesh=finer,
        in_specs=(brick, brick, brick, P("gx", GY, GZ, None), brick, P(), P(), P(), P(), P()),
        out_specs=(brick, brick, P(), P(), P(AXES, None)),
        check_vma=False,
    )
```
